128 devices in a mesh: table: 32 (over y, x, core), tensor: 4 (over z).
Axes of the slice: x: 4, y: 4, z: 4, core: 2. Of those that a mesh axis runs over, the one named last changes fastest.
Arguments:
- hidden: bfloat16 [1024, 2560], P('table'), may hold values from -16 to 16
- attn_gain: float32 [2560], replicated, may hold values from 0.6 to 1.4
- q_weight: bfloat16 [2560, 2560], P(None, 'tensor'), may hold values from -1 to 1
- kv_weight: bfloat16 [2560, 2, 512], P(None, None, 'tensor'), may hold values from -0.125 to 0.125
- out_weight: bfloat16 [2560, 2560], P('tensor'), may hold values from -0.125 to 0.125
- key_cache: bfloat16 [1024, 256, 512], P('table', None, 'tensor'), may hold values from -256 to 256
- value_cache: bfloat16 [1024, 256, 512], P('table', None, 'tensor'), may hold values from -6 to 6
- cache_lengths: int32 [1024], P('table'), may hold values from 64 to 256
- table: bfloat16 [131072, 1280], P('table'), may hold values from -6 to 6
- key_proj: bfloat16 [1280, 2560], P(None, 'tensor'), may hold values from -0.15625 to 0.15625
- value_proj: bfloat16 [1280, 2560], P(None, 'tensor'), may hold values from -0.15625 to 0.15625
- lookup_ids: int32 [1024, 16], P('table'), may hold values from 0 to 131071, as said below
Outputs:
- mixed: bfloat16 [1024, 2560], P('table', 'tensor')
The draws below stay inside these ranges and needn't reach their ends.
Inputs may be any that keep to these rules, and one draw needn't show every extreme that they name: `lookup_ids`: within the 32 sequences of one index of table (aligned blocks of rows), at most 32 ids lie in the range of 4096 rows of any one owner (owner = id // 4096); in every draw one owner gets exactly 32 ids from every block.
All inputs are finite; a program needn't handle non-finite values.
Results may differ from the reference program's by a relative error of at most 0.007.
Values may be sent and summed in bfloat16 or wider, within the bound.
No kernel may reach another device: no remote copies, remote signals or barrier semaphores. Data moves between devices by JAX's collectives and lax.ppermute only.
A program may use at most 128 MiB of HBM per device.

```python
import math
import jax
import jax.numpy as jnp
from jax import lax

D = 2560
EMB = 1280
HEADS = 20
KV_HEADS = 4
HEAD_DIM = 128
LOOKUPS = 16
SEQ_DEV = 32
CTX = 256
ROWS_DEV = 4096
SEQS = 1024
ROWS = 131072
CAP = 32
N_TABLE = 32


def joint_draw(key):
    base_key = jax.random.fold_in(key, 5)
    subkeys = jax.random.split(base_key, 6)
    col_scale = jnp.exp(jax.random.uniform(subkeys[0], (1, D), jnp.float32, math.log(0.5), math.log(2.0)))
    hidden = jax.random.normal(subkeys[1], (SEQS, D), jnp.float32) * col_scale
    hidden = jnp.clip(hidden, -16.0, 16.0)
    gain_draw = jax.random.uniform(subkeys[3], (D,), jnp.float32, 0.6, 1.4)
    query_weight = jnp.clip(jax.random.normal(subkeys[4], (D, HEADS * HEAD_DIM), jnp.float32) / math.sqrt(D), -1.0, 1.0)
    key_draw = jax.random.normal(subkeys[5], (SEQS, CTX, KV_HEADS * HEAD_DIM), jnp.float32)
    key_draw = jnp.clip(key_draw, -256.0, 256.0)
    return (hidden, gain_draw, query_weight, key_draw)


def draw_hidden(key, part):
    return joint_draw(key)[0].astype(jnp.bfloat16)


def draw_attn_gain(key, part):
    return joint_draw(key)[1].astype(jnp.float32)


def draw_q_weight(key, part):
    return joint_draw(key)[2].astype(jnp.bfloat16)


def draw_key_cache(key, part):
    return joint_draw(key)[3].astype(jnp.bfloat16)


def draw_lookup_ids(key, part):
    base_key = jax.random.fold_in(key, 11)
    subkeys = jax.random.split(base_key, 4)
    requests = SEQ_DEV * LOOKUPS
    position_total = N_TABLE * CAP
    heaviest_holder = jax.random.randint(subkeys[0], (), 0, N_TABLE)
    position_number = jnp.arange(position_total, dtype=jnp.int32)
    holder_by_position = position_number // CAP
    energy_offset = jnp.where(holder_by_position == heaviest_holder, 1 << 17, 0).astype(jnp.int32)
    attention_energies = jax.random.randint(subkeys[1], (N_TABLE, position_total), 0, 1 << 16)
    combined_result = (attention_energies + energy_offset[None, :]) * position_total + position_number[None, :]
    picked = lax.top_k(combined_result, requests)[1]
    owner_of = (picked // CAP).astype(jnp.int32)
    shuffle_keys = jax.random.randint(subkeys[2], (N_TABLE, requests), 0, 1 << 16) * requests + jnp.arange(requests, dtype=jnp.int32)[None, :]
    positions = jnp.argsort(shuffle_keys, axis=1)
    owner_of = jnp.take_along_axis(owner_of, positions, axis=1)
    local_row = jax.random.randint(subkeys[3], (N_TABLE, requests), 0, ROWS_DEV)
    return (owner_of * ROWS_DEV + local_row).reshape(N_TABLE * SEQ_DEV, LOOKUPS).astype(jnp.int32)


def plant(result, stream_key, low, largest):
    place = [jax.random.randint(jax.random.fold_in(stream_key, axis), (), 0, length) for axis, length in enumerate(result.shape)]
    main_axis = result.shape.index(max(result.shape))
    next_to = place[:main_axis] + [(place[main_axis] + 1) % result.shape[main_axis]] + place[main_axis + 1:]
    return result.at[tuple(place)].set(low).at[tuple(next_to)].set(largest)


def steps_of(stream_key, extent, shards, low, top_value):
    factor_of = 1.0
    for position, shards_of in shards:
        steps = jax.random.uniform(jax.random.fold_in(jax.random.fold_in(stream_key, 6), position), (shards_of,), jnp.float32, low / len(shards), top_value / len(shards))
        factor_of = factor_of * jnp.repeat(jnp.exp(steps), extent[position] // shards_of).reshape((-1,) + (1,) * (len(extent) - 1 - position))
    return factor_of


def centred(rng, shape, deviation, most, shards=(), kind=jnp.bfloat16):
    drawn = jax.random.normal(rng, shape, jnp.float32) * deviation
    if len(shards) > 0:
        drawn = steps_of(rng, shape, shards, -0.22, 0.18) * drawn
    return jnp.clip(drawn, min=-most, max=most).astype(kind)


def setup_inputs(seed: int = 0) -> dict:
    key_of = jax.random.split(jax.random.key(seed), 13)
    hidden = draw_hidden(jax.random.fold_in(key_of[12], 71), 0)
    attn_gain = draw_attn_gain(jax.random.fold_in(key_of[12], 71), 0)
    q_weight = draw_q_weight(jax.random.fold_in(key_of[12], 71), 0)
    kv_weight = centred(key_of[3], (D, 2, KV_HEADS * HEAD_DIM), D ** -0.5, 0.125, ((2, 4),))
    out_weight = centred(key_of[4], (HEADS * HEAD_DIM, D), (HEADS * HEAD_DIM) ** -0.5, 0.125, ((0, 4),))
    key_cache = draw_key_cache(jax.random.fold_in(key_of[12], 71), 0)
    value_cache = centred(key_of[6], (SEQS, CTX, KV_HEADS * HEAD_DIM), 1.0, 6.0, ((0, 32), (2, 4)))
    cache_lengths = plant(jax.random.randint(key_of[7], (SEQS,), CTX // 4, CTX + 1), jax.random.fold_in(key_of[7], 1), CTX // 4, CTX).astype(jnp.int32)
    table = centred(key_of[8], (ROWS, EMB), 1.0, 6.0, ((0, 32),))
    key_proj = centred(key_of[9], (EMB, D), EMB ** -0.5, 0.15625, ((1, 4),))
    value_proj = centred(key_of[10], (EMB, D), EMB ** -0.5, 0.15625, ((1, 4),))
    lookup_ids = draw_lookup_ids(jax.random.fold_in(key_of[12], 71), 0)
    return {"hidden": hidden, "attn_gain": attn_gain, "q_weight": q_weight, "kv_weight": kv_weight, "out_weight": out_weight, "key_cache": key_cache, "value_cache": value_cache, "cache_lengths": cache_lengths, "table": table, "key_proj": key_proj, "value_proj": value_proj, "lookup_ids": lookup_ids}


epsilon = 1e-06

def attend(sequence_item):
    query_heads, new_key, new_value, key_rows, value_rows, length = sequence_item
    group_size = HEADS // KV_HEADS
    inv_scale = 1.0 / math.sqrt(HEAD_DIM)
    query_f = query_heads.astype(jnp.float32).reshape(KV_HEADS, group_size, HEAD_DIM)
    key_f = key_rows.astype(jnp.float32)
    value_f = value_rows.astype(jnp.float32)
    attention_energies = jnp.einsum('kgh,ckh->kgc', query_f, key_f) * inv_scale
    own_score = jnp.einsum('kgh,kh->kg', query_f, new_key.astype(jnp.float32)) * inv_scale
    valid_mask = jnp.arange(CTX, dtype=jnp.int32) < length
    masked = jnp.where(valid_mask[None, None, :], attention_energies, -1e+30)
    row_max = jnp.maximum(lax.optimization_barrier(jnp.max(masked, axis=-1)), own_score)
    weights = jnp.exp(masked - row_max[..., None])
    own_weight = jnp.exp(own_score - row_max)
    denom_sum = lax.optimization_barrier(jnp.sum(weights, axis=-1)) + own_weight
    weights_bf = (weights / denom_sum[..., None]).astype(jnp.bfloat16)
    own_prob = (own_weight / denom_sum).astype(jnp.bfloat16)
    context = jnp.einsum('kgc,ckh->kgh', weights_bf.astype(jnp.float32), value_f)
    context = context + own_prob.astype(jnp.float32)[..., None] * new_value.astype(jnp.float32)[:, None, :]
    return context.reshape(HEADS * HEAD_DIM).astype(jnp.bfloat16)

def reference(hidden, attn_gain, q_weight, kv_weight, out_weight, key_cache, value_cache, cache_lengths, table, key_proj, value_proj, lookup_ids):
    hidden_f32 = hidden.astype(jnp.float32)
    normed = hidden_f32 * lax.rsqrt(lax.optimization_barrier(jnp.mean(hidden_f32 * hidden_f32, axis=1, keepdims=True)) + epsilon)
    attn_in = (normed * attn_gain).astype(jnp.bfloat16)
    query_proj = jnp.dot(attn_in, q_weight, preferred_element_type=jnp.float32).astype(jnp.bfloat16)
    query_proj = query_proj.reshape(SEQS, HEADS, HEAD_DIM)
    kv_cols = KV_HEADS * HEAD_DIM
    new_kv = jnp.dot(attn_in, kv_weight.reshape(D, 2 * kv_cols), preferred_element_type=jnp.float32).astype(jnp.bfloat16)
    new_key = new_kv[:, :kv_cols].reshape(SEQS, KV_HEADS, HEAD_DIM)
    new_value = new_kv[:, kv_cols:].reshape(SEQS, KV_HEADS, HEAD_DIM)
    key_rows = key_cache.reshape(SEQS, CTX, KV_HEADS, HEAD_DIM)
    value_rows = value_cache.reshape(SEQS, CTX, KV_HEADS, HEAD_DIM)
    context = lax.map(attend, (query_proj, new_key, new_value, key_rows, value_rows, cache_lengths))
    attention = jnp.dot(context, out_weight, preferred_element_type=jnp.float32)
    rows = table[lookup_ids.reshape(-1)]
    mem_key = jnp.dot(rows, key_proj, preferred_element_type=jnp.float32).reshape(SEQS, LOOKUPS, D)
    mem_value = jnp.dot(rows, value_proj, preferred_element_type=jnp.float32).reshape(SEQS, LOOKUPS, D)
    cross_term = lax.optimization_barrier(jnp.sum(mem_key * normed[:, None, :], axis=-1))
    square_sum = lax.optimization_barrier(jnp.sum(mem_key * mem_key, axis=-1))
    gating = jax.nn.sigmoid(cross_term * lax.rsqrt(square_sum / D + epsilon) / math.sqrt(D))
    memory = lax.optimization_barrier(jnp.sum(gating[..., None] * mem_value, axis=1))
    return (hidden_f32 + attention + memory).astype(jnp.bfloat16)
```

```python
import math

import jax
import jax.numpy as jnp
from jax import lax
from jax.experimental import pallas as pl
from jax.experimental.pallas import tpu as pltpu
from jax.sharding import PartitionSpec as P

HEAD_DIM = 128
EPS = 1e-06
LANES = 128
F32 = jnp.float32
BF16 = jnp.bfloat16
I32 = jnp.int32


def iota(shape, dim):
    return lax.broadcasted_iota(I32, shape, dim)


def ones_where(mask):
    return jnp.where(mask, 1.0, 0.0).astype(BF16)


def mm(a, b):
    return lax.dot_general(a, b, (((1,), (0,)), ((), ())), preferred_element_type=F32)


def mm_nt(a, b):
    return lax.dot_general(a, b, (((1,), (1,)), ((), ())), preferred_element_type=F32)


def mm_tn(a, b):
    return lax.dot_general(a, b, (((0,), (0,)), ((), ())), preferred_element_type=F32)


def two_parts(x):
    high = x.astype(BF16)
    return high, (x - high.astype(F32)).astype(BF16)


def three_parts(x):
    high = x.astype(BF16)
    rest = x - high.astype(F32)
    mid = rest.astype(BF16)
    return high, mid, (rest - mid.astype(F32)).astype(BF16)


def exact_int_mm(left, value):
    return 64.0 * mm(left, (value >> 6).astype(F32).astype(BF16)) + mm(
        left, (value & 63).astype(F32).astype(BF16)
    )


def send_ids_kernel(ids_ref, out_ref):
    peers = out_ref.shape[0]
    out_ref[...] = jnp.broadcast_to(ids_ref[...][None], (peers, *ids_ref.shape))


def slot_map_kernel(first_ref, ids_ref, map_ref, *, rows_dev, owners, seqs, lookups, slots):
    requests = seqs * lookups
    owner = ids_ref[...] // rows_dev
    hit = ones_where(iota((owners, requests), 0) == owner)
    before = ones_where(iota((requests, requests), 0) < iota((requests, requests), 1))
    count = mm(hit, before)
    rank = jnp.sum(count * hit.astype(F32), axis=0, keepdims=True).astype(I32)
    rel = rank - first_ref[0]
    slot = jnp.where((rel >= 0) & (rel < slots), owner * slots + rel, -1)
    placed = ones_where(iota((owners * slots, requests), 0) == slot)
    of_seq = ones_where(iota((seqs, requests), 1) // lookups == iota((seqs, requests), 0))
    map_ref[...] = mm_nt(placed, of_seq).astype(BF16)


def squares_kernel(table_ref, key_ref, out_ref):
    keys = mm(table_ref[...], key_ref[...])
    width = keys.shape[1]
    folded = keys[:, :LANES] * keys[:, :LANES]
    for c in range(LANES, width, LANES):
        part = keys[:, c : c + LANES]
        folded = folded + part * part
    for g in range(keys.shape[0] // LANES):
        block = folded[g * LANES : (g + 1) * LANES, :]
        out_ref[0, g : g + 1, :] = jnp.sum(block.T, axis=0, keepdims=True)


def gather_kernel(
    where_ref, got_ref, table_ref, rows_ref, ids_ref, col_ref, acc_ref, *, rows_dev, askers, slots
):
    step = pl.program_id(0)
    per = got_ref.shape[0] // askers
    total = got_ref.shape[0]
    n_slots = askers * slots

    @pl.when(step == 0)
    def _():
        local = got_ref[...] - where_ref[0] * rows_dev
        mine = (local >= 0) & (local < rows_dev)
        hit = ones_where(mine)
        before = ones_where(iota((LANES, LANES), 0) < iota((LANES, LANES), 1))
        r, c = iota((total, total), 0), iota((total, total), 1)
        earlier = ones_where((r // per == c // per) & (c < r))
        rank = mm(hit, before) + jnp.sum(mm(earlier, hit), axis=1, keepdims=True)
        rel = jnp.where(mine, rank.astype(I32) - where_ref[1], -1)
        lane = iota((total, LANES), 1)
        picked = jnp.zeros((total, LANES), I32)
        for k in range(slots):
            one = jnp.sum(jnp.where(rel == k, local, 0).astype(F32), axis=1, keepdims=True)
            picked = jnp.where(lane == k, one.astype(I32), picked)
        same = ones_where(
            iota((n_slots, total), 1) // per == iota((n_slots, total), 0) // slots
        )
        spread = exact_int_mm(same, picked)
        keep = iota((n_slots, LANES), 1) == iota((n_slots, LANES), 0) % slots
        col = jnp.sum(jnp.where(keep, spread, 0.0), axis=1, keepdims=True).astype(I32)
        col_ref[...] = jnp.broadcast_to(col, (n_slots, LANES))
        ids_ref[...] = jnp.broadcast_to(col, (n_slots, LANES))
        acc_ref[...] = jnp.zeros_like(acc_ref)

    block = table_ref.shape[0]
    col = col_ref[:, :1] - step * block
    chosen = ones_where(iota((n_slots, block), 1) == col)
    acc_ref[...] += mm(chosen, table_ref[...])

    @pl.when(step == pl.num_programs(0) - 1)
    def _():
        rows_ref[...] = acc_ref[...].astype(BF16)


def pick_squares_kernel(ids_ref, sq_ref, out_ref, *, slots):
    ids = ids_ref[...]
    n_slots = ids.shape[0]
    groups = sq_ref.shape[0]
    rowsel = ones_where(iota((n_slots, groups), 1) == ids[:, :1] // LANES)
    high, mid, low = three_parts(sq_ref[...])
    wide = mm(rowsel, high) + (mm(rowsel, mid) + mm(rowsel, low))
    lane = iota((n_slots, LANES), 1)
    value = jnp.sum(jnp.where(lane == ids % LANES, wide, 0.0), axis=1, keepdims=True)
    placed = jnp.where(lane == iota((n_slots, LANES), 0) % slots, value, 0.0)
    out_ref[...] = jnp.sum(placed.reshape(n_slots // slots, slots, LANES), axis=1)


def mix_kernel(rows_ref, map_ref, u_ref, sq_ref, attn_ref, out_ref, *, slots, width):
    rows = rows_ref[...]
    n_slots = rows.shape[0]
    of_seq = map_ref[...].astype(F32)
    u_high, u_low = two_parts(u_ref[...])
    cross_all = mm_nt(rows, u_high) + mm_nt(rows, u_low)
    cross = jnp.sum(cross_all * of_seq, axis=1, keepdims=True)
    owners = sq_ref.shape[0]
    spread = jnp.broadcast_to(sq_ref[...][:, None, :], (owners, slots, LANES)).reshape(n_slots, LANES)
    keep = iota((n_slots, LANES), 1) == iota((n_slots, LANES), 0) % slots
    square = jnp.sum(jnp.where(keep, spread, 0.0), axis=1, keepdims=True)
    gate = jax.nn.sigmoid(cross * lax.rsqrt(square / width + EPS) / math.sqrt(width))
    g_high, g_low = two_parts(of_seq * gate)
    mixed = (mm_tn(g_high, rows) + mm_tn(g_low, rows)).astype(BF16)
    peers, _, out_width = out_ref.shape
    part = width // peers
    for p in range(peers):
        out_ref[p, :, :part] = attn_ref[:, p * part : (p + 1) * part]
        out_ref[p, :, part:] = mixed


def final_kernel(got_ref, value_ref, hidden_ref, out_ref):
    part = out_ref.shape[1]
    total = got_ref[0].astype(F32)
    for p in range(1, got_ref.shape[0]):
        total = total + got_ref[p].astype(F32)
    high, low = two_parts(total[:, part:])
    memory = mm(high, value_ref[...]) + mm(low, value_ref[...])
    out_ref[...] = (hidden_ref[...].astype(F32) + total[:, :part] + memory).astype(BF16)


def whole(shape):
    return pl.BlockSpec(shape, lambda *_: (0,) * len(shape))


def butterfly(x, axis):
    peers = lax.axis_size(axis)
    step = 1
    while step < peers:
        x = x + lax.ppermute(x, axis, [(i, i ^ step) for i in range(peers)])
        step *= 2
    return x


def attention_part(hidden_f32, normed, attn_gain, q_weight, kv_weight, out_weight, key_cache, value_cache, cache_lengths):
    seq_count, width = hidden_f32.shape
    attn_in = (normed * attn_gain).astype(BF16)
    ctx_len = key_cache.shape[1]
    kv_width = kv_weight.shape[2]
    kv_local = kv_width // HEAD_DIM
    group_size = q_weight.shape[1] // kv_width
    inv_scale = 1.0 / math.sqrt(HEAD_DIM)
    query_proj = jnp.dot(attn_in, q_weight, preferred_element_type=F32).astype(BF16)
    new_kv = jnp.dot(
        attn_in, kv_weight.reshape(width, 2 * kv_width), preferred_element_type=F32
    ).astype(BF16)
    query_heads = query_proj.reshape(seq_count, kv_local, group_size, HEAD_DIM)
    new_key = new_kv[:, :kv_width].reshape(seq_count, kv_local, HEAD_DIM)
    new_value = new_kv[:, kv_width:].reshape(seq_count, kv_local, HEAD_DIM)
    key_blocks = key_cache.reshape(seq_count, ctx_len, kv_local, HEAD_DIM)
    value_blocks = value_cache.reshape(seq_count, ctx_len, kv_local, HEAD_DIM)
    energies = (
        jnp.einsum("skgh,sckh->skgc", query_heads, key_blocks, preferred_element_type=F32)
        * inv_scale
    )
    own_score = (
        jnp.einsum("skgh,skh->skg", query_heads, new_key, preferred_element_type=F32) * inv_scale
    )
    valid = jnp.arange(ctx_len, dtype=I32)[None, :] < cache_lengths[:, None]
    masked = jnp.where(valid[:, None, None, :], energies, -1e30)
    row_max = jnp.maximum(jnp.max(masked, axis=-1), own_score)
    weights = jnp.exp(masked - row_max[..., None])
    own_weight = jnp.exp(own_score - row_max)
    denom = jnp.sum(weights, axis=-1) + own_weight
    weights_bf = (weights / denom[..., None]).astype(BF16)
    own_prob = (own_weight / denom).astype(BF16)
    context = jnp.einsum("skgc,sckh->skgh", weights_bf, value_blocks, preferred_element_type=F32)
    context = context + own_prob.astype(F32)[..., None] * new_value.astype(F32)[:, :, None, :]
    context = context.reshape(seq_count, -1).astype(BF16)
    return jnp.dot(context, out_weight, preferred_element_type=F32).astype(BF16)


def local(
    hidden,
    attn_gain,
    q_weight,
    kv_weight,
    out_weight,
    key_cache,
    value_cache,
    cache_lengths,
    table,
    key_proj,
    value_proj,
    lookup_ids,
):
    seqs, width = hidden.shape
    lookups = lookup_ids.shape[1]
    requests = seqs * lookups
    rows_dev, emb = table.shape
    owners = lax.axis_size("table")
    tensor = lax.axis_size("tensor")
    me_table, me_tensor = lax.axis_index("table"), lax.axis_index("tensor")
    part = width // tensor
    capacity = 2 * requests // owners
    slots = capacity // tensor
    n_slots = owners * slots
    per = requests // LANES

    ids_flat = lookup_ids.reshape(requests)
    send = pl.pallas_call(
        send_ids_kernel,
        out_shape=jax.ShapeDtypeStruct((owners, per, LANES), I32),
        name="send_ids",
    )(ids_flat.reshape(per, LANES))
    got_ids = lax.all_to_all(send, "table", 0, 0, tiled=True)

    first = (me_tensor * slots).astype(I32)
    slot_map = pl.pallas_call(
        lambda *refs: slot_map_kernel(
            *refs, rows_dev=rows_dev, owners=owners, seqs=seqs, lookups=lookups, slots=slots
        ),
        out_shape=jax.ShapeDtypeStruct((n_slots, seqs), BF16),
        in_specs=[pl.BlockSpec(memory_space=pltpu.SMEM), pl.BlockSpec(memory_space=pltpu.VMEM)],
        name="slot_map",
    )(first.reshape(1), ids_flat.reshape(1, requests))

    hidden_f32 = hidden.astype(F32)
    normed = hidden_f32 * lax.rsqrt(jnp.mean(hidden_f32 * hidden_f32, axis=1, keepdims=True) + EPS)
    normed_slice = lax.dynamic_slice_in_dim(normed, me_tensor * part, part, 1)
    n_high, n_low = two_parts(normed_slice)
    u = mm_nt(n_high, key_proj) + mm_nt(n_low, key_proj)
    u = butterfly(u, "tensor")

    block = 512
    squares = pl.pallas_call(
        squares_kernel,
        grid=(rows_dev // block,),
        in_specs=[pl.BlockSpec((block, emb), lambda i: (i, 0)), whole(key_proj.shape)],
        out_specs=pl.BlockSpec((1, block // LANES, LANES), lambda i: (i, 0, 0)),
        out_shape=jax.ShapeDtypeStruct((rows_dev // block, block // LANES, LANES), F32),
        name="squares",
    )(table, key_proj)
    squares = butterfly(squares.reshape(rows_dev // LANES, LANES), "tensor")

    rows, row_ids = pl.pallas_call(
        lambda *refs: gather_kernel(*refs, rows_dev=rows_dev, askers=owners, slots=slots),
        grid=(rows_dev // block,),
        in_specs=[
            pl.BlockSpec(memory_space=pltpu.SMEM),
            whole((owners * per, LANES)),
            pl.BlockSpec((block, emb), lambda i: (i, 0)),
        ],
        out_specs=[whole((n_slots, emb)), whole((n_slots, LANES))],
        out_shape=[
            jax.ShapeDtypeStruct((n_slots, emb), BF16),
            jax.ShapeDtypeStruct((n_slots, LANES), I32),
        ],
        scratch_shapes=[pltpu.VMEM((n_slots, LANES), I32), pltpu.VMEM((n_slots, emb), F32)],
        name="gather_rows",
    )(jnp.stack([me_table.astype(I32), first]), got_ids.reshape(owners * per, LANES), table)
    got_rows = lax.all_to_all(rows.reshape(owners, slots, emb), "table", 0, 0, tiled=True)

    picked = pl.pallas_call(
        lambda *refs: pick_squares_kernel(*refs, slots=slots),
        out_shape=jax.ShapeDtypeStruct((owners, LANES), F32),
        name="pick_squares",
    )(row_ids, squares)
    got_squares = lax.all_to_all(picked.reshape(owners, 1, LANES), "table", 0, 0, tiled=True)

    attention = attention_part(
        hidden_f32, normed, attn_gain, q_weight, kv_weight, out_weight, key_cache, value_cache, cache_lengths
    )

    mixes = pl.pallas_call(
        lambda *refs: mix_kernel(*refs, slots=slots, width=width),
        out_shape=jax.ShapeDtypeStruct((tensor, seqs, part + emb), BF16),
        name="mix",
    )(got_rows.reshape(n_slots, emb), slot_map, u, got_squares.reshape(owners, LANES), attention)
    got_mixes = lax.all_to_all(mixes, "tensor", 0, 0, tiled=True)

    hidden_slice = lax.dynamic_slice_in_dim(hidden, me_tensor * part, part, 1)
    return pl.pallas_call(
        final_kernel,
        out_shape=jax.ShapeDtypeStruct((seqs, part), BF16),
        name="final",
    )(got_mixes, value_proj, hidden_slice)


def solution(mesh):
    return jax.shard_map(
        local,
        mesh=mesh,
        in_specs=(
            P("table", None),
            P(),
            P(None, "tensor"),
            P(None, None, "tensor"),
            P("tensor", None),
            P("table", None, "tensor"),
            P("table", None, "tensor"),
            P("table"),
            P("table", None),
            P(None, "tensor"),
            P(None, "tensor"),
            P("table", None),
        ),
        out_specs=P("table", "tensor"),
        check_vma=False,
    )
```

```python
import math

import jax
import jax.numpy as jnp
from jax import lax
from jax.experimental import pallas as pl
from jax.experimental.pallas import tpu as pltpu
from jax.sharding import PartitionSpec as P


HEAD_DIM = 128
EPS = 1e-06
LANES = 128
F32 = jnp.float32
BF16 = jnp.bfloat16
I32 = jnp.int32


def iota(shape, dim):
    return lax.broadcasted_iota(I32, shape, dim)


def ones_where(mask):
    return jnp.where(mask, 1.0, 0.0).astype(BF16)


def mm(a, b):
    return lax.dot_general(a, b, (((1,), (0,)), ((), ())), preferred_element_type=F32)


def mm_nt(a, b):
    return lax.dot_general(a, b, (((1,), (1,)), ((), ())), preferred_element_type=F32)


def mm_tn(a, b):
    return lax.dot_general(a, b, (((0,), (0,)), ((), ())), preferred_element_type=F32)


def two_parts(x):
    high = x.astype(BF16)
    return high, (x - high.astype(F32)).astype(BF16)


def three_parts(x):
    high = x.astype(BF16)
    rest = x - high.astype(F32)
    mid = rest.astype(BF16)
    return high, mid, (rest - mid.astype(F32)).astype(BF16)


def send_ids_kernel(ids_ref, out_ref):
    _, per, _ = out_ref.shape
    _, seqs = ids_ref.shape
    fit = LANES // seqs
    flat = [
        jnp.concatenate([ids_ref[j * fit + q : j * fit + q + 1, :] for q in range(fit)], axis=1)
        for j in range(per)
    ]
    flat = jnp.concatenate(flat, axis=0)
    out_ref[...] = jnp.broadcast_to(flat[None], out_ref.shape)


def slot_map_kernel(first_ref, ids_ref, map_ref, *, rows_dev, owners, seqs, lookups, slots):
    requests = seqs * lookups
    ids = jnp.concatenate([ids_ref[j : j + 1, :] for j in range(lookups)], axis=1)
    owner = ids // rows_dev
    hit = ones_where(iota((owners, requests), 0) == owner)
    before = ones_where(iota((requests, requests), 0) < iota((requests, requests), 1))
    count = mm(hit, before)
    rank = jnp.sum(count * hit.astype(F32), axis=0, keepdims=True).astype(I32)
    rel = rank - first_ref[0]
    slot = jnp.where((rel >= 0) & (rel < slots), owner * slots + rel, -1)
    placed = ones_where(iota((owners * slots, requests), 0) == slot)
    of_seq = ones_where(iota((seqs, requests), 1) % seqs == iota((seqs, requests), 0))
    map_ref[...] = mm_nt(placed, of_seq).astype(BF16)


def squares_kernel(
    z_ref, hidden_ref, gain_ref, table_ref, key_ref, order_ref, out_ref, attn_in_ref, u_ref
):
    del order_ref
    sub = 256

    @pl.when(pl.program_id(0) == 0)
    def _():
        part = key_ref.shape[1]
        hidden = hidden_ref[...].astype(F32)
        inv = lax.rsqrt(jnp.mean(hidden * hidden, axis=1, keepdims=True) + EPS)
        attn_in_ref[...] = (hidden * inv * gain_ref[...]).astype(BF16)
        start = pl.multiple_of(z_ref[0] * part, LANES)
        high, low = two_parts(hidden_ref[:, pl.ds(start, part)].astype(F32) * inv)
        u_ref[...] = (mm_nt(high, key_ref[...]) + mm_nt(low, key_ref[...])).astype(BF16)

    for t in range(table_ref.shape[0] // sub):
        keys = mm(table_ref[t * sub : (t + 1) * sub, :], key_ref[...])
        folded = keys[:, :LANES] * keys[:, :LANES]
        for c in range(LANES, keys.shape[1], LANES):
            part = keys[:, c : c + LANES]
            folded = folded + part * part
        for g in range(sub // LANES):
            block = folded[g * LANES : (g + 1) * LANES, :]
            row = t * (sub // LANES) + g
            out_ref[0, row : row + 1, :] = jnp.sum(block.T, axis=0, keepdims=True)


def slot_lanes(row, z, slots):
    askers = row.shape[0]
    lane = iota((askers, LANES), 1)
    own = row if z == 0 else pltpu.roll(row, LANES - z * slots, 1)
    own = jnp.where(lane < slots, own, 0.0)
    step = slots
    while step < LANES:
        own = own + pltpu.roll(own, step, 1)
        step *= 2
    fit = LANES // slots
    own = jnp.where(lane // slots == iota((askers, LANES), 0) % fit, own, 0.0)
    return jnp.sum(own.reshape(askers // fit, fit, LANES), axis=1)


def select_kernel(
    where_ref, got_ref, sq_ref, u_ref, idx_ref, out_ref, *, rows_dev, per, capacity, tensor
):
    groups = sq_ref.shape[0]
    askers = got_ref.shape[0] // per
    seqs = u_ref.shape[0]
    slots = capacity // tensor
    before = ones_where(iota((LANES, LANES), 0) < iota((LANES, LANES), 1))
    lane = iota((askers, LANES), 1)
    seen = jnp.zeros((askers, 1), F32)
    ranks, locals_ = [], []
    for j in range(per):
        local = got_ref[pl.ds(j, askers, stride=per), :] - where_ref[0] * rows_dev
        mine = (local >= 0) & (local < rows_dev)
        rank = mm(ones_where(mine), before) + seen
        seen = seen + jnp.sum(jnp.where(mine, 1.0, 0.0), axis=1, keepdims=True)
        ranks.append(jnp.where(mine, rank, -1.0).astype(I32))
        locals_.append(local.astype(F32))
    row = jnp.zeros((askers, LANES), F32)
    for k in range(capacity):
        one = jnp.where(ranks[0] == k, locals_[0], 0.0)
        for j in range(1, per):
            one = one + jnp.where(ranks[j] == k, locals_[j], 0.0)
        row = jnp.where(lane == k, jnp.sum(one, axis=1, keepdims=True), row)
    idx = jnp.zeros(idx_ref.shape, F32)
    for z in range(tensor):
        idx = jnp.where(where_ref[1] == z, slot_lanes(row, z, slots), idx)
    idx_ref[...] = idx.astype(I32)
    ids = row.astype(I32)
    high, low = ids // LANES, ids % LANES
    value = jnp.zeros((askers, LANES), F32)
    for g in range(groups):
        line = jnp.broadcast_to(sq_ref[g : g + 1, :], (askers, LANES))
        found = jnp.take_along_axis(line, low, axis=1, mode="promise_in_bounds")
        value = jnp.where(high == g, found, value)
    u = u_ref[...]
    for z in range(tensor):
        out_ref[z, :seqs, :] = u
        out_ref[z, seqs:, :] = jnp.zeros((out_ref.shape[1] - seqs, u.shape[1]), BF16)
        lines = slot_lanes(value, z, slots)
        for p, part in enumerate(three_parts(lines)):
            out_ref[z, seqs : seqs + lines.shape[0], p * LANES : (p + 1) * LANES] = part


def pack_kernel(rows_ref, got_ref, out_ref, *, seqs):
    owners, slots, _ = out_ref.shape
    n_slots, emb = rows_ref.shape
    lines = n_slots // LANES
    total = jnp.zeros((lines, LANES), F32)
    for p in range(3):
        for z in range(got_ref.shape[0]):
            total = total + got_ref[z, seqs : seqs + 8, p * LANES : (p + 1) * LANES].astype(F32)[:lines]
    spread = jnp.concatenate(
        [jnp.broadcast_to(total[i : i + 1, :], (LANES, LANES)) for i in range(lines)], axis=0
    )
    lane = iota((n_slots, LANES), 1)
    keep = lane == iota((n_slots, LANES), 0) % LANES
    column = jnp.sum(jnp.where(keep, spread, 0.0), axis=1, keepdims=True)
    extra = jnp.zeros((n_slots, LANES), F32)
    for p, part in enumerate(three_parts(column)):
        extra = jnp.where(lane == p, part.astype(F32), extra)
    out_ref[:, :, :emb] = rows_ref[...].reshape(owners, slots, emb)
    out_ref[:, :, emb:] = extra.astype(BF16).reshape(owners, slots, LANES)


def attention_kernel(
    lens_ref, x_ref, qw_hbm, kvw_hbm, key_hbm, val_hbm, ow_hbm, out_ref,
    qw, kvw, key, val, ow, sems,
):
    seqs, width = x_ref.shape
    ctx_len = key_hbm.shape[1]
    heads = qw_hbm.shape[1] // HEAD_DIM
    pad = 8
    copies = [
        pltpu.make_async_copy(src, dst, sems.at[i])
        for i, (src, dst) in enumerate(
            ((qw_hbm, qw), (kvw_hbm, kvw), (key_hbm, key), (val_hbm, val), (ow_hbm, ow))
        )
    ]
    for copy in copies:
        copy.start()
    x = x_ref[...]
    copies[0].wait()
    query = mm(x, qw[...]).astype(BF16)
    src, dst = iota((HEAD_DIM, 4 * HEAD_DIM), 0), iota((HEAD_DIM, 4 * HEAD_DIM), 1)
    spread = ones_where(dst - jnp.where(dst < 2 * HEAD_DIM, 0, 2 * HEAD_DIM + 1) == 2 * src)
    blocks = width // HEAD_DIM
    stacked = jnp.concatenate(
        [x[:, g * HEAD_DIM : (g + 1) * HEAD_DIM] for g in range(blocks)], axis=0
    )
    wide = mm(stacked, spread).astype(BF16)
    even = jnp.concatenate(
        [wide[g * seqs : (g + 1) * seqs, : 2 * HEAD_DIM] for g in range(blocks)], axis=1
    )
    odd = jnp.concatenate(
        [wide[g * seqs : (g + 1) * seqs, 2 * HEAD_DIM :] for g in range(blocks)], axis=1
    )
    copies[1].wait()
    new_kv = mm(jnp.concatenate([even, odd], axis=0), kvw[...]).astype(BF16)
    rows = seqs * pad
    r, c = iota((rows, seqs), 0), iota((rows, seqs), 1)
    q_rows = jnp.zeros((rows, HEAD_DIM), F32)
    for g in range(heads):
        put = ones_where((r // pad == c) & (r % pad == g))
        q_rows = q_rows + mm(put, query[:, g * HEAD_DIM : (g + 1) * HEAD_DIM])
    rep = ones_where(r // pad == c)
    new_key = mm(rep, new_kv[:seqs, :])
    new_value = mm(rep, new_kv[seqs:, :])
    inv_scale = 1.0 / math.sqrt(HEAD_DIM)
    own = jnp.sum(q_rows * new_key, axis=1, keepdims=True) * inv_scale
    copies[2].wait()
    place = iota((pad, ctx_len), 1)
    energies = []
    for s in range(seqs):
        q_s = q_rows[s * pad : (s + 1) * pad, :].astype(BF16)
        score = mm_nt(q_s, key[s]) * inv_scale
        energies.append(jnp.where(place < lens_ref[s], score, -1e30))
    energies = jnp.concatenate(energies, axis=0)
    top = jnp.maximum(jnp.max(energies, axis=1, keepdims=True), own)
    weights = jnp.exp(energies - top)
    own_weight = jnp.exp(own - top)
    denom = jnp.sum(weights, axis=1, keepdims=True) + own_weight
    probs = weights / denom
    own_prob = (own_weight / denom).astype(BF16).astype(F32)
    copies[3].wait()
    context = []
    for s in range(seqs):
        context.append(mm(probs[s * pad : (s + 1) * pad, :].astype(BF16), val[s]))
    context = (jnp.concatenate(context, axis=0) + own_prob * new_value).astype(BF16)
    r, c = iota((seqs, rows), 0), iota((seqs, rows), 1)
    flat = []
    for g in range(heads):
        take = ones_where((c // pad == r) & (c % pad == g))
        flat.append(mm(take, context).astype(BF16))
    copies[4].wait()
    out_ref[...] = mm(jnp.concatenate(flat, axis=1), ow[...]).astype(BF16)


def mix_kernel(rows_ref, map_ref, got_ref, attn_ref, out_ref, *, width):
    _, seqs = map_ref.shape
    emb = got_ref.shape[2]
    rows = rows_ref[:, :emb]
    of_seq = map_ref[...].astype(F32)
    u = got_ref[0, :seqs, :].astype(F32)
    for z in range(1, got_ref.shape[0]):
        u = u + got_ref[z, :seqs, :].astype(F32)
    u_high, u_low = two_parts(u)
    cross_all = mm_nt(rows, u_high) + mm_nt(rows, u_low)
    cross = jnp.sum(cross_all * of_seq, axis=1, keepdims=True)
    square = jnp.sum(rows_ref[:, emb:].astype(F32), axis=1, keepdims=True)
    gate = jax.nn.sigmoid(cross * lax.rsqrt(square / width + EPS) / math.sqrt(width))
    g_high, g_low = two_parts(of_seq * gate)
    mixed = (mm_tn(g_high, rows) + mm_tn(g_low, rows)).astype(BF16)
    peers, _, _ = out_ref.shape
    part = width // peers
    for p in range(peers):
        out_ref[p, :, :part] = attn_ref[:, p * part : (p + 1) * part]
        out_ref[p, :, part:] = mixed


def final_kernel(got_ref, value_ref, hidden_ref, out_ref):
    part = out_ref.shape[1]
    total = got_ref[0].astype(F32)
    for p in range(1, got_ref.shape[0]):
        total = total + got_ref[p].astype(F32)
    high, low = two_parts(total[:, part:])
    memory = mm(high, value_ref[...]) + mm(low, value_ref[...])
    out_ref[...] = (hidden_ref[...].astype(F32) + total[:, :part] + memory).astype(BF16)


def whole(shape):
    return pl.BlockSpec(shape, lambda *_: (0,) * len(shape))


def body(
    hidden,
    attn_gain,
    q_weight,
    kv_weight,
    out_weight,
    key_cache,
    value_cache,
    cache_lengths,
    table,
    key_proj,
    value_proj,
    lookup_ids,
):
    seqs, width = hidden.shape
    lookups = lookup_ids.shape[1]
    requests = seqs * lookups
    rows_dev, emb = table.shape
    owners = lax.axis_size("table")
    tensor = lax.axis_size("tensor")
    me_table, me_tensor = lax.axis_index("table"), lax.axis_index("tensor")
    part = width // tensor
    capacity = 2 * requests // owners
    slots = capacity // tensor
    n_slots = owners * slots
    per = requests // LANES

    vmem = pl.BlockSpec(memory_space=pltpu.VMEM)
    smem = pl.BlockSpec(memory_space=pltpu.SMEM)
    hbm = pl.BlockSpec(memory_space=pl.ANY)
    ids_t = lookup_ids.T

    send = pl.pallas_call(
        send_ids_kernel,
        out_shape=jax.ShapeDtypeStruct((owners, per, LANES), I32),
        name="send_ids",
    )(ids_t)
    got_ids = lax.all_to_all(send, "table", 0, 0, tiled=True)

    block = 512
    squares, attn_in, u_part = pl.pallas_call(
        squares_kernel,
        grid=(rows_dev // block,),
        in_specs=[
            smem,
            whole(hidden.shape),
            whole((1, width)),
            pl.BlockSpec((block, emb), lambda i: (i, 0)),
            whole(key_proj.shape),
            hbm,
        ],
        out_specs=[
            pl.BlockSpec((1, block // LANES, LANES), lambda i: (i, 0, 0)),
            whole(hidden.shape),
            whole((seqs, emb)),
        ],
        out_shape=[
            jax.ShapeDtypeStruct((rows_dev // block, block // LANES, LANES), F32),
            jax.ShapeDtypeStruct(hidden.shape, BF16),
            jax.ShapeDtypeStruct((seqs, emb), BF16),
        ],
        name="squares",
    )(me_tensor.astype(I32).reshape(1), hidden, attn_gain.reshape(1, width), table, key_proj, send)

    where = jnp.stack([me_table.astype(I32), me_tensor.astype(I32)])
    idx, shares = pl.pallas_call(
        lambda *refs: select_kernel(
            *refs, rows_dev=rows_dev, per=per, capacity=capacity, tensor=tensor
        ),
        in_specs=[smem, vmem, vmem, vmem],
        out_shape=[
            jax.ShapeDtypeStruct((n_slots // LANES, LANES), I32),
            jax.ShapeDtypeStruct((tensor, seqs + 8, emb), BF16),
        ],
        name="select",
    )(where, got_ids.reshape(owners * per, LANES), squares.reshape(rows_dev // LANES, LANES), u_part)
    got_shares = lax.all_to_all(shares, "tensor", 0, 0, tiled=True)
    rows = table.at[idx.reshape(n_slots)].get(mode="promise_in_bounds")

    first = (me_tensor * slots).astype(I32)
    slot_map = pl.pallas_call(
        lambda *refs: slot_map_kernel(
            *refs, rows_dev=rows_dev, owners=owners, seqs=seqs, lookups=lookups, slots=slots
        ),
        out_shape=jax.ShapeDtypeStruct((n_slots, seqs), BF16),
        in_specs=[smem, vmem],
        name="slot_map",
    )(first.reshape(1), ids_t)

    packed = pl.pallas_call(
        lambda *refs: pack_kernel(*refs, seqs=seqs),
        out_shape=jax.ShapeDtypeStruct((owners, slots, emb + LANES), BF16),
        name="pack",
    )(rows, got_shares)
    got_rows = lax.all_to_all(packed, "table", 0, 0, tiled=True)

    _, kv_width = key_cache.shape[1:]
    attention = pl.pallas_call(
        attention_kernel,
        in_specs=[smem, vmem, hbm, hbm, hbm, hbm, hbm],
        out_shape=jax.ShapeDtypeStruct((seqs, width), BF16),
        scratch_shapes=[
            pltpu.VMEM(q_weight.shape, BF16),
            pltpu.VMEM((2 * width, kv_width), BF16),
            pltpu.VMEM(key_cache.shape, BF16),
            pltpu.VMEM(value_cache.shape, BF16),
            pltpu.VMEM(out_weight.shape, BF16),
            pltpu.SemaphoreType.DMA((5,)),
        ],
        name="attention",
    )(
        cache_lengths, attn_in, q_weight, kv_weight.reshape(2 * width, kv_width),
        key_cache, value_cache, out_weight,
    )

    mixes = pl.pallas_call(
        lambda *refs: mix_kernel(*refs, width=width),
        out_shape=jax.ShapeDtypeStruct((tensor, seqs, part + emb), BF16),
        name="mix",
    )(got_rows.reshape(n_slots, emb + LANES), slot_map, got_shares, attention)
    got_mixes = lax.all_to_all(mixes, "tensor", 0, 0, tiled=True)

    hidden_slice = lax.dynamic_slice_in_dim(hidden, me_tensor * part, part, 1)
    return pl.pallas_call(
        final_kernel,
        out_shape=jax.ShapeDtypeStruct((seqs, part), BF16),
        name="final",
    )(got_mixes, value_proj, hidden_slice)


def solution(mesh):
    return jax.shard_map(
        body,
        mesh=mesh,
        in_specs=(
            P("table", None),
            P(),
            P(None, "tensor"),
            P(None, None, "tensor"),
            P("tensor", None),
            P("table", None, "tensor"),
            P("table", None, "tensor"),
            P("table"),
            P("table", None),
            P(None, "tensor"),
            P(None, "tensor"),
            P("table", None),
        ),
        out_specs=P("table", "tensor"),
        check_vma=False,
    )
```

```python
import math

import jax
import jax.numpy as jnp
from jax import lax
from jax.experimental import pallas as pl
from jax.experimental.pallas import tpu as pltpu
from jax.sharding import PartitionSpec as P


HEAD_DIM = 128
EPS = 1e-06
LANES = 128
F32 = jnp.float32
BF16 = jnp.bfloat16
I32 = jnp.int32


def iota(shape, dim):
    return lax.broadcasted_iota(I32, shape, dim)


def ones_where(mask):
    return jnp.where(mask, 1.0, 0.0).astype(BF16)


def mm(a, b):
    return lax.dot_general(a, b, (((1,), (0,)), ((), ())), preferred_element_type=F32)


def mm_nt(a, b):
    return lax.dot_general(a, b, (((1,), (1,)), ((), ())), preferred_element_type=F32)


def mm_tn(a, b):
    return lax.dot_general(a, b, (((0,), (0,)), ((), ())), preferred_element_type=F32)


def two_parts(x):
    high = x.astype(BF16)
    return high, (x - high.astype(F32)).astype(BF16)


def three_parts(x):
    high = x.astype(BF16)
    rest = x - high.astype(F32)
    mid = rest.astype(BF16)
    return high, mid, (rest - mid.astype(F32)).astype(BF16)


def send_ids_kernel(ids_ref, out_ref):
    _, per, _ = out_ref.shape
    _, seqs = ids_ref.shape
    fit = LANES // seqs
    flat = [
        jnp.concatenate([ids_ref[j * fit + q : j * fit + q + 1, :] for q in range(fit)], axis=1)
        for j in range(per)
    ]
    flat = jnp.concatenate(flat, axis=0)
    out_ref[...] = jnp.broadcast_to(flat[None], out_ref.shape)


def slot_map_kernel(first_ref, ids_ref, map_ref, *, rows_dev, owners, seqs, lookups, slots):
    requests = seqs * lookups
    ids = jnp.concatenate([ids_ref[j : j + 1, :] for j in range(lookups)], axis=1)
    owner = ids // rows_dev
    hit = ones_where(iota((owners, requests), 0) == owner)
    before = ones_where(iota((requests, requests), 0) < iota((requests, requests), 1))
    count = mm(hit, before)
    rank = jnp.sum(count * hit.astype(F32), axis=0, keepdims=True).astype(I32)
    rel = rank - first_ref[0]
    slot = jnp.where((rel >= 0) & (rel < slots), owner * slots + rel, -1)
    placed = ones_where(iota((owners * slots, requests), 0) == slot)
    of_seq = ones_where(iota((seqs, requests), 1) % seqs == iota((seqs, requests), 0))
    map_ref[...] = mm_nt(placed, of_seq).astype(BF16)


def squares_kernel(
    z_ref, gain_ref, hidden_hbm, key_hbm, table_hbm, order_ref, out_ref, attn_in_ref,
    hidden_ref, key_ref, table, key_t, squares, sems, *, chunks,
):
    del order_ref
    sub = 256
    early = [
        pltpu.make_async_copy(hidden_hbm, hidden_ref, sems.at[len(chunks)]),
        pltpu.make_async_copy(key_hbm, key_ref, sems.at[len(chunks) + 1]),
    ]
    for copy in early:
        copy.start()
    copies, start = [], 0
    for i, size in enumerate(chunks):
        rows = pl.ds(start, size)
        copies.append(pltpu.make_async_copy(table_hbm.at[rows, :], table.at[rows, :], sems.at[i]))
        copies[-1].start()
        start += size
    part = key_ref.shape[1]
    seqs = hidden_ref.shape[0]
    early[0].wait()
    hidden = hidden_ref[...].astype(F32)
    inv = lax.rsqrt(jnp.mean(hidden * hidden, axis=1, keepdims=True) + EPS)
    attn_in_ref[...] = (hidden * inv * gain_ref[...].reshape(1, hidden.shape[1])).astype(BF16)
    first = pl.multiple_of(z_ref[0] * part, LANES)
    high, low = two_parts(hidden_ref[:, pl.ds(first, part)].astype(F32) * inv)
    early[1].wait()
    key_t[...] = key_ref[...].T
    u = mm(jnp.concatenate([high, low], axis=0), key_t[...])
    u = (u[:seqs] + u[seqs:]).astype(BF16)
    start = 0
    for copy, size in zip(copies, chunks):
        copy.wait()
        for t in range(start, start + size, sub):
            keys = mm_nt(key_t[...], table[t : t + sub, :])
            line = jnp.sum(keys * keys, axis=0, keepdims=True)
            for g in range(sub // LANES):
                squares[t // LANES + g : t // LANES + g + 1, :] = line[:, g * LANES : (g + 1) * LANES]
        start += size
    peers, lines, emb = out_ref.shape
    tail = lines - seqs
    parts = three_parts(squares[...])
    pieces = [p[h : h + tail] for p in parts for h in range(0, squares.shape[0], tail)]
    rest = emb - LANES * len(pieces)
    block = jnp.concatenate(pieces + [jnp.zeros((tail, rest), BF16)], axis=1)
    for p in range(peers):
        out_ref[p, :seqs, :] = u
        out_ref[p, seqs:, :] = block


def slot_lanes(row, z, slots):
    askers = row.shape[0]
    lane = iota((askers, LANES), 1)
    own = row if z == 0 else pltpu.roll(row, LANES - z * slots, 1)
    own = jnp.where(lane < slots, own, 0.0)
    step = slots
    while step < LANES:
        own = own + pltpu.roll(own, step, 1)
        step *= 2
    fit = LANES // slots
    own = jnp.where(lane // slots == iota((askers, LANES), 0) % fit, own, 0.0)
    return jnp.sum(own.reshape(askers // fit, fit, LANES), axis=1)


def gather_kernel(
    me_ref, z_ref, got_ref, table_hbm, rows_ref, ids_ref, idx_vmem, idx_smem, groups, sems,
    *, rows_dev, per, capacity, tensor,
):
    askers = got_ref.shape[0] // per
    slots = capacity // tensor
    before = ones_where(iota((LANES, LANES), 0) < iota((LANES, LANES), 1))
    lane = iota((askers, LANES), 1)
    seen = jnp.zeros((askers, 1), F32)
    low_rank = z_ref[0] * slots
    ranks, locals_ = [], []
    for j in range(per):
        local = got_ref[pl.ds(j, askers, stride=per), :] - me_ref[0] * rows_dev
        mine = (local >= 0) & (local < rows_dev)
        rank = mm(ones_where(mine), before) + seen
        seen = seen + jnp.sum(jnp.where(mine, 1.0, 0.0), axis=1, keepdims=True)
        ranks.append(jnp.where(mine, rank.astype(I32) - low_rank, -1))
        locals_.append(local.astype(F32))
    row = jnp.zeros((askers, LANES), F32)
    for k in range(slots):
        one = jnp.where(ranks[0] == k, locals_[0], 0.0)
        for j in range(1, per):
            one = one + jnp.where(ranks[j] == k, locals_[j], 0.0)
        row = jnp.where(lane == k, jnp.sum(one, axis=1, keepdims=True), row)
    ids_ref[...] = row.astype(I32)
    idx_vmem[...] = slot_lanes(row, 0, slots).astype(I32)
    to_smem = pltpu.make_async_copy(idx_vmem, idx_smem, sems.at[0])
    to_smem.start()
    n_slots = askers * slots
    spread = jnp.broadcast_to(row.astype(I32)[:, None, :], (askers, slots, LANES))
    spread = spread.reshape(n_slots, LANES)
    keep = iota((n_slots, LANES), 1) == iota((n_slots, LANES), 0) % slots
    column = jnp.sum(jnp.where(keep, spread % 8, 0).astype(F32), axis=1, keepdims=True)
    to_smem.wait()
    for h in range(n_slots // LANES):
        def issue(i, carry):
            base = pl.multiple_of((idx_smem[h, i] // 8) * 8, 8)
            place = pl.multiple_of((h * LANES + i) * 8, 8)
            pltpu.make_async_copy(
                table_hbm.at[pl.ds(base, 8), :], groups.at[pl.ds(place, 8), :], sems.at[1]
            ).start()
            return carry

        lax.fori_loop(0, LANES, issue, 0, unroll=8)
    pltpu.make_async_copy(table_hbm.at[pl.ds(0, n_slots * 8), :], groups, sems.at[1]).wait()
    size = 32
    for b in range(n_slots // size):
        offset = iota((size, size * 8), 1) - 8 * iota((size, size * 8), 0)
        pick = ones_where(offset.astype(F32) == column[b * size : (b + 1) * size, :])
        rows_ref[b * size : (b + 1) * size, :] = mm(
            pick, groups[b * size * 8 : (b + 1) * size * 8, :]
        ).astype(BF16)


def pack_kernel(rows_ref, ids_ref, got_ref, out_ref, *, seqs):
    owners, slots, _ = out_ref.shape
    n_slots, emb = rows_ref.shape
    tail = got_ref.shape[1] - seqs
    per_part = 32 // tail
    halves = []
    for h in range(per_part):
        total = jnp.zeros((tail, LANES), F32)
        for p in range(3):
            c = (p * per_part + h) * LANES
            for z in range(got_ref.shape[0]):
                total = total + got_ref[z, seqs:, c : c + LANES].astype(F32)
        halves.append(total)
    squares = jnp.concatenate(halves, axis=0)
    ids = ids_ref[...]
    high, low = ids // LANES, ids % LANES
    value = jnp.zeros(ids.shape, F32)
    for g in range(squares.shape[0]):
        line = jnp.broadcast_to(squares[g : g + 1, :], ids.shape)
        found = jnp.take_along_axis(line, low, axis=1, mode="promise_in_bounds")
        value = jnp.where(high == g, found, value)
    spread = jnp.broadcast_to(value[:, None, :], (owners, slots, LANES)).reshape(n_slots, LANES)
    lane = iota((n_slots, LANES), 1)
    keep = lane == iota((n_slots, LANES), 0) % slots
    column = jnp.sum(jnp.where(keep, spread, 0.0), axis=1, keepdims=True)
    extra = jnp.zeros((n_slots, LANES), F32)
    for p, part in enumerate(three_parts(column)):
        extra = jnp.where(lane == p, part.astype(F32), extra)
    out_ref[:, :, :emb] = rows_ref[...].reshape(owners, slots, emb)
    out_ref[:, :, emb:] = extra.astype(BF16).reshape(owners, slots, LANES)


def attention_kernel(
    lens_ref, first_ref, ids_ref, x_ref, qw_hbm, kvw_hbm, key_hbm, val_hbm, ow_hbm,
    out_ref, map_ref, qw, kvw, key, val, ow, sems, *, mapping,
):
    seqs, width = x_ref.shape
    ctx_len = key_hbm.shape[1]
    heads = qw_hbm.shape[1] // HEAD_DIM
    pad = 8
    copies = [
        pltpu.make_async_copy(src, dst, sems.at[i])
        for i, (src, dst) in enumerate(
            (
                (qw_hbm, qw),
                (kvw_hbm, kvw),
                (key_hbm, key),
                (val_hbm, val),
                (ow_hbm, ow),
            )
        )
    ]
    for copy in copies:
        copy.start()
    slot_map_kernel(first_ref, ids_ref, map_ref, **mapping)
    x = x_ref[...]
    copies[0].wait()
    query = mm(x, qw[...]).astype(BF16)
    src, dst = iota((HEAD_DIM, 4 * HEAD_DIM), 0), iota((HEAD_DIM, 4 * HEAD_DIM), 1)
    spread = ones_where(dst - jnp.where(dst < 2 * HEAD_DIM, 0, 2 * HEAD_DIM + 1) == 2 * src)
    blocks = width // HEAD_DIM
    stacked = jnp.concatenate(
        [x[:, g * HEAD_DIM : (g + 1) * HEAD_DIM] for g in range(blocks)], axis=0
    )
    wide = mm(stacked, spread).astype(BF16)
    even = jnp.concatenate(
        [wide[g * seqs : (g + 1) * seqs, : 2 * HEAD_DIM] for g in range(blocks)], axis=1
    )
    odd = jnp.concatenate(
        [wide[g * seqs : (g + 1) * seqs, 2 * HEAD_DIM :] for g in range(blocks)], axis=1
    )
    copies[1].wait()
    new_kv = mm(jnp.concatenate([even, odd], axis=0), kvw[...]).astype(BF16)
    rows = seqs * pad
    r, c = iota((rows, seqs), 0), iota((rows, seqs), 1)
    q_rows = jnp.zeros((rows, HEAD_DIM), F32)
    for g in range(heads):
        put = ones_where((r // pad == c) & (r % pad == g))
        q_rows = q_rows + mm(put, query[:, g * HEAD_DIM : (g + 1) * HEAD_DIM])
    rep = ones_where(r // pad == c)
    new_key = mm(rep, new_kv[:seqs, :])
    new_value = mm(rep, new_kv[seqs:, :])
    inv_scale = 1.0 / math.sqrt(HEAD_DIM)
    own = jnp.sum(q_rows * new_key, axis=1, keepdims=True) * inv_scale
    copies[2].wait()
    place = iota((pad, ctx_len), 1)
    energies = []
    for s in range(seqs):
        q_s = q_rows[s * pad : (s + 1) * pad, :].astype(BF16)
        score = mm_nt(q_s, key[s]) * inv_scale
        energies.append(jnp.where(place < lens_ref[s], score, -1e30))
    energies = jnp.concatenate(energies, axis=0)
    top = jnp.maximum(jnp.max(energies, axis=1, keepdims=True), own)
    weights = jnp.exp(energies - top)
    own_weight = jnp.exp(own - top)
    denom = jnp.sum(weights, axis=1, keepdims=True) + own_weight
    probs = weights / denom
    own_prob = (own_weight / denom).astype(BF16).astype(F32)
    copies[3].wait()
    context = []
    for s in range(seqs):
        context.append(mm(probs[s * pad : (s + 1) * pad, :].astype(BF16), val[s]))
    context = (jnp.concatenate(context, axis=0) + own_prob * new_value).astype(BF16)
    r, c = iota((seqs, rows), 0), iota((seqs, rows), 1)
    flat = []
    for g in range(heads):
        take = ones_where((c // pad == r) & (c % pad == g))
        flat.append(mm(take, context).astype(BF16))
    copies[4].wait()
    out_ref[...] = mm(jnp.concatenate(flat, axis=1), ow[...]).astype(BF16)


def mix_kernel(rows_ref, map_ref, got_ref, attn_ref, out_ref, *, width):
    _, seqs = map_ref.shape
    emb = got_ref.shape[2]
    rows = rows_ref[:, :emb]
    of_seq = map_ref[...].astype(F32)
    u = got_ref[0, :seqs, :].astype(F32)
    for z in range(1, got_ref.shape[0]):
        u = u + got_ref[z, :seqs, :].astype(F32)
    u_high, u_low = two_parts(u)
    cross_all = mm_nt(rows, u_high) + mm_nt(rows, u_low)
    cross = jnp.sum(cross_all * of_seq, axis=1, keepdims=True)
    square = jnp.sum(rows_ref[:, emb:].astype(F32), axis=1, keepdims=True)
    gate = jax.nn.sigmoid(cross * lax.rsqrt(square / width + EPS) / math.sqrt(width))
    g_high, g_low = two_parts(of_seq * gate)
    mixed = (mm_tn(g_high, rows) + mm_tn(g_low, rows)).astype(BF16)
    peers, _, _ = out_ref.shape
    part = width // peers
    for p in range(peers):
        out_ref[p, :, :part] = attn_ref[:, p * part : (p + 1) * part]
        out_ref[p, :, part:] = mixed


def fetch_kernel(value_hbm, hidden_hbm, order_ref, value_ref, hidden_ref, sems):
    del order_ref
    copies = [
        pltpu.make_async_copy(value_hbm, value_ref, sems.at[0]),
        pltpu.make_async_copy(hidden_hbm, hidden_ref, sems.at[1]),
    ]
    for copy in copies:
        copy.start()
    for copy in copies:
        copy.wait()


def final_kernel(z_ref, got_ref, value_ref, hidden_ref, out_ref):
    part = out_ref.shape[1]
    first = pl.multiple_of(z_ref[0] * part, LANES)
    total = got_ref[0].astype(F32)
    for p in range(1, got_ref.shape[0]):
        total = total + got_ref[p].astype(F32)
    high, low = two_parts(total[:, part:])
    memory = mm(high, value_ref[...]) + mm(low, value_ref[...])
    out_ref[...] = (hidden_ref[:, pl.ds(first, part)].astype(F32) + total[:, :part] + memory).astype(BF16)


def body(
    hidden,
    attn_gain,
    q_weight,
    kv_weight,
    out_weight,
    key_cache,
    value_cache,
    cache_lengths,
    table,
    key_proj,
    value_proj,
    lookup_ids,
):
    seqs, width = hidden.shape
    lookups = lookup_ids.shape[1]
    requests = seqs * lookups
    rows_dev, emb = table.shape
    owners = lax.axis_size("table")
    tensor = lax.axis_size("tensor")
    me_table, me_tensor = lax.axis_index("table"), lax.axis_index("tensor")
    part = width // tensor
    capacity = 2 * requests // owners
    slots = capacity // tensor
    n_slots = owners * slots
    per = requests // LANES

    vmem = pl.BlockSpec(memory_space=pltpu.VMEM)
    smem = pl.BlockSpec(memory_space=pltpu.SMEM)
    hbm = pl.BlockSpec(memory_space=pl.ANY)
    ids_t = lookup_ids.T

    send = pl.pallas_call(
        send_ids_kernel,
        out_shape=jax.ShapeDtypeStruct((owners, per, LANES), I32),
        name="send_ids",
    )(ids_t)
    got_ids = lax.all_to_all(send, "table", 0, 0, tiled=True)

    def near(x):
        return pltpu.with_memory_space_constraint(x, pltpu.VMEM)

    me = me_table.astype(I32).reshape(1)
    z = me_tensor.astype(I32).reshape(1)
    chunks = (256, 256, 512, 1024, 1024, 1024)
    shares, attn_in = pl.pallas_call(
        lambda *refs: squares_kernel(*refs, chunks=chunks),
        in_specs=[smem, vmem, hbm, hbm, hbm, hbm],
        out_specs=[vmem, vmem],
        out_shape=[
            jax.ShapeDtypeStruct((tensor, seqs + 16, emb), BF16),
            jax.ShapeDtypeStruct(hidden.shape, BF16),
        ],
        scratch_shapes=[
            pltpu.VMEM(hidden.shape, BF16),
            pltpu.VMEM(key_proj.shape, BF16),
            pltpu.VMEM(table.shape, BF16),
            pltpu.VMEM((part, emb), BF16),
            pltpu.VMEM((rows_dev // LANES, LANES), F32),
            pltpu.SemaphoreType.DMA((len(chunks) + 2,)),
        ],
        name="squares",
    )(z, attn_gain, hidden, key_proj, table, send)
    got_shares = lax.all_to_all(shares, "tensor", 0, 0, tiled=True)

    rows, row_ids = pl.pallas_call(
        lambda *refs: gather_kernel(
            *refs, rows_dev=rows_dev, per=per, capacity=capacity, tensor=tensor
        ),
        in_specs=[smem, smem, vmem, hbm],
        out_specs=[vmem, vmem],
        out_shape=[pltpu.VMEM((n_slots, emb), BF16), pltpu.VMEM((owners, LANES), I32)],
        scratch_shapes=[
            pltpu.VMEM((n_slots // LANES, LANES), I32),
            pltpu.SMEM((n_slots // LANES, LANES), I32),
            pltpu.VMEM((n_slots * 8, emb), BF16),
            pltpu.SemaphoreType.DMA((2,)),
        ],
        name="gather",
    )(me, z, near(got_ids.reshape(owners * per, LANES)), table)

    near_shares = near(got_shares)
    packed = pl.pallas_call(
        lambda *refs: pack_kernel(*refs, seqs=seqs),
        in_specs=[vmem] * 3,
        out_specs=vmem,
        out_shape=jax.ShapeDtypeStruct((owners, slots, emb + LANES), BF16),
        name="pack",
    )(near(rows), near(row_ids), near_shares)
    got_rows = lax.all_to_all(packed, "table", 0, 0, tiled=True)

    _, kv_width = key_cache.shape[1:]
    mapping = dict(rows_dev=rows_dev, owners=owners, seqs=seqs, lookups=lookups, slots=slots)
    attention, slot_map = pl.pallas_call(
        lambda *refs: attention_kernel(*refs, mapping=mapping),
        in_specs=[smem, smem, vmem, vmem, hbm, hbm, hbm, hbm, hbm],
        out_specs=[vmem, vmem],
        out_shape=[
            pltpu.VMEM((seqs, width), BF16),
            pltpu.VMEM((n_slots, seqs), BF16),
        ],
        scratch_shapes=[
            pltpu.VMEM(q_weight.shape, BF16),
            pltpu.VMEM((2 * width, kv_width), BF16),
            pltpu.VMEM(key_cache.shape, BF16),
            pltpu.VMEM(value_cache.shape, BF16),
            pltpu.VMEM(out_weight.shape, BF16),
            pltpu.SemaphoreType.DMA((5,)),
        ],
        name="attention",
    )(
        cache_lengths, z * slots, ids_t, attn_in, q_weight,
        kv_weight.reshape(2 * width, kv_width), key_cache, value_cache, out_weight,
    )

    mixes = pl.pallas_call(
        lambda *refs: mix_kernel(*refs, width=width),
        in_specs=[vmem] * 4,
        out_specs=vmem,
        out_shape=jax.ShapeDtypeStruct((tensor, seqs, part + emb), BF16),
        name="mix",
    )(near(got_rows.reshape(n_slots, emb + LANES)), near(slot_map), near_shares, near(attention))
    got_mixes = lax.all_to_all(mixes, "tensor", 0, 0, tiled=True)

    value_near, hidden_near = pl.pallas_call(
        fetch_kernel,
        in_specs=[hbm] * 3,
        out_specs=[vmem] * 2,
        out_shape=[pltpu.VMEM(value_proj.shape, BF16), pltpu.VMEM(hidden.shape, BF16)],
        scratch_shapes=[pltpu.SemaphoreType.DMA((2,))],
        name="fetch_value",
    )(value_proj, hidden, mixes)

    return pl.pallas_call(
        final_kernel,
        in_specs=[smem] + [vmem] * 3,
        out_specs=vmem,
        out_shape=jax.ShapeDtypeStruct((seqs, part), BF16),
        name="final",
    )(z, near(got_mixes), near(value_near), near(hidden_near))


def solution(mesh):
    return jax.shard_map(
        body,
        mesh=mesh,
        in_specs=(
            P("table", None),
            P(),
            P(None, "tensor"),
            P(None, None, "tensor"),
            P("tensor", None),
            P("table", None, "tensor"),
            P("table", None, "tensor"),
            P("table"),
            P("table", None),
            P(None, "tensor"),
            P(None, "tensor"),
            P("table", None),
        ),
        out_specs=P("table", "tensor"),
        check_vma=False,
    )
```

```python
import math

import jax
import jax.numpy as jnp
from jax import lax
from jax.experimental import pallas as pl
from jax.experimental.pallas import tpu as pltpu
from jax.sharding import PartitionSpec as P


HEAD_DIM = 128
EPS = 1e-06
LANES = 128
F32 = jnp.float32
BF16 = jnp.bfloat16
I32 = jnp.int32


def iota(shape, dim):
    return lax.broadcasted_iota(I32, shape, dim)


def ones_where(mask):
    return jnp.where(mask, 1.0, 0.0).astype(BF16)


def mm(a, b):
    return lax.dot_general(a, b, (((1,), (0,)), ((), ())), preferred_element_type=F32)


def mm_nt(a, b):
    return lax.dot_general(a, b, (((1,), (1,)), ((), ())), preferred_element_type=F32)


def mm_tn(a, b):
    return lax.dot_general(a, b, (((0,), (0,)), ((), ())), preferred_element_type=F32)


def two_parts(x):
    high = x.astype(BF16)
    return high, (x - high.astype(F32)).astype(BF16)


def three_parts(x):
    high = x.astype(BF16)
    rest = x - high.astype(F32)
    mid = rest.astype(BF16)
    return high, mid, (rest - mid.astype(F32)).astype(BF16)


def send_ids_kernel(ids_ref, out_ref):
    _, per, _ = out_ref.shape
    _, seqs = ids_ref.shape
    fit = LANES // seqs
    flat = [
        jnp.concatenate([ids_ref[j * fit + q : j * fit + q + 1, :] for q in range(fit)], axis=1)
        for j in range(per)
    ]
    flat = jnp.concatenate(flat, axis=0)
    out_ref[...] = jnp.broadcast_to(flat[None], out_ref.shape)


def slot_map_kernel(z_ref, ids_ref, map_ref, *, rows_dev, owners, seqs, lookups, capacity, tensor):
    requests = seqs * lookups
    total, width = map_ref.shape
    ids = jnp.concatenate([ids_ref[j : j + 1, :] for j in range(lookups)], axis=1)
    owner = ids // rows_dev
    hit = ones_where(iota((owners, requests), 0) == owner)
    before = ones_where(iota((requests, requests), 0) < iota((requests, requests), 1))
    rank = jnp.sum(mm(hit, before) * hit.astype(F32), axis=0, keepdims=True).astype(I32)
    key = owner * capacity + rank - z_ref[0] * (capacity // tensor)
    row = iota((total, requests), 0)
    place = row % capacity
    placed = ones_where(row - place + (place // 8) * 2 + place % 2 == key)
    of_seq = ones_where(iota((width, requests), 1) % seqs == iota((width, requests), 0) % seqs)
    part = (iota((total, width), 0) % 8) // 2
    known = mm_nt(placed, of_seq)
    map_ref[...] = jnp.where(part == iota((total, width), 1) // seqs, known, 0.0).astype(BF16)


def squares_kernel(
    z_ref, gain_ref, hidden_hbm, key_hbm, table_hbm, order_ref, squares, u_ref, attn_in_ref,
    hidden_ref, key_ref, table, key_t, sems, *, chunks,
):
    del order_ref
    sub = 256
    early = [
        pltpu.make_async_copy(hidden_hbm, hidden_ref, sems.at[len(chunks)]),
        pltpu.make_async_copy(key_hbm, key_ref, sems.at[len(chunks) + 1]),
    ]
    for copy in early:
        copy.start()
    copies, start = [], 0
    for i, size in enumerate(chunks):
        rows = pl.ds(start, size)
        copies.append(pltpu.make_async_copy(table_hbm.at[rows, :], table.at[rows, :], sems.at[i]))
        copies[-1].start()
        start += size
    part = key_ref.shape[1]
    seqs = hidden_ref.shape[0]
    early[0].wait()
    hidden = hidden_ref[...].astype(F32)
    inv = lax.rsqrt(jnp.mean(hidden * hidden, axis=1, keepdims=True) + EPS)
    attn_in_ref[...] = (hidden * inv * gain_ref[...].reshape(1, hidden.shape[1])).astype(BF16)
    first = pl.multiple_of(z_ref[0] * part, LANES)
    high, low = two_parts(hidden_ref[:, pl.ds(first, part)].astype(F32) * inv)
    early[1].wait()
    key_t[...] = key_ref[...].T
    u = mm(jnp.concatenate([high, low], axis=0), key_t[...])
    u_ref[...] = (u[:seqs] + u[seqs:]).astype(BF16)
    start = 0
    for copy, size in zip(copies, chunks):
        copy.wait()
        for t in range(start, start + size, sub):
            keys = mm_nt(key_t[...], table[t : t + sub, :])
            line = jnp.sum(keys * keys, axis=0, keepdims=True)
            for g in range(sub // LANES):
                squares[t // LANES + g : t // LANES + g + 1, :] = line[:, g * LANES : (g + 1) * LANES]
        start += size


def slot_lanes(row, z, slots):
    askers = row.shape[0]
    lane = iota((askers, LANES), 1)
    own = row if z == 0 else pltpu.roll(row, LANES - z * slots, 1)
    own = jnp.where(lane < slots, own, 0.0)
    step = slots
    while step < LANES:
        own = own + pltpu.roll(own, step, 1)
        step *= 2
    fit = LANES // slots
    own = jnp.where(lane // slots == iota((askers, LANES), 0) % fit, own, 0.0)
    return jnp.sum(own.reshape(askers // fit, fit, LANES), axis=1)


def gather_kernel(
    me_ref, z_ref, got_ref, sq_ref, table_hbm, out_ref, idx_vmem, idx_smem, groups, sems,
    *, rows_dev, per, capacity, tensor,
):
    askers = got_ref.shape[0] // per
    slots = capacity // tensor
    n_slots = askers * slots
    before = ones_where(iota((LANES, LANES), 0) < iota((LANES, LANES), 1))
    lane = iota((askers, LANES), 1)
    seen = jnp.zeros((askers, 1), F32)
    ranks, locals_ = [], []
    for j in range(per):
        local = got_ref[pl.ds(j, askers, stride=per), :] - me_ref[0] * rows_dev
        mine = (local >= 0) & (local < rows_dev)
        rank = mm(ones_where(mine), before) + seen
        seen = seen + jnp.sum(jnp.where(mine, 1.0, 0.0), axis=1, keepdims=True)
        ranks.append(jnp.where(mine, rank, -1.0).astype(I32))
        locals_.append(local.astype(F32))
    row = jnp.zeros((askers, LANES), F32)
    for k in range(capacity):
        one = jnp.where(ranks[0] == k, locals_[0], 0.0)
        for j in range(1, per):
            one = one + jnp.where(ranks[j] == k, locals_[j], 0.0)
        row = jnp.where(lane == k, jnp.sum(one, axis=1, keepdims=True), row)
    moved = row
    for z in range(1, tensor):
        moved = jnp.where(z_ref[0] == z, pltpu.roll(row, LANES - 2 * z, 1), moved)
    own = jnp.zeros((askers, LANES), F32)
    for z in range(tensor):
        piece = moved if z == 0 else pltpu.roll(moved, LANES - (slots - 2) * z, 1)
        own = jnp.where(lane // 2 == z, piece, own)
    idx_vmem[...] = slot_lanes(own, 0, slots).astype(I32)
    to_smem = pltpu.make_async_copy(idx_vmem, idx_smem, sems.at[0])
    to_smem.start()
    to_smem.wait()
    for h in range(n_slots // LANES):
        def issue(i, carry):
            base = pl.multiple_of((idx_smem[h, i] // 8) * 8, 8)
            place = pl.multiple_of((h * LANES + i) * 8, 8)
            pltpu.make_async_copy(
                table_hbm.at[pl.ds(base, 8), :], groups.at[pl.ds(place, 8), :], sems.at[1]
            ).start()
            return carry

        lax.fori_loop(0, LANES, issue, 0, unroll=8)
    ids = row.astype(I32)
    high, low = ids // LANES, ids % LANES
    value = jnp.zeros((askers, LANES), F32)
    for g in range(sq_ref.shape[0]):
        line = jnp.broadcast_to(sq_ref[g : g + 1, :], (askers, LANES))
        found = jnp.take_along_axis(line, low, axis=1, mode="promise_in_bounds")
        value = jnp.where(high == g, found, value)
    extra = []
    for z in range(tensor):
        piece = value if z == 0 else pltpu.roll(value, LANES - slots * z, 1)
        line = jnp.zeros((askers, LANES), F32)
        for p, part in enumerate(three_parts(jnp.where(lane < slots, piece, 0.0))):
            part = part.astype(F32)
            line = line + (part if p == 0 else pltpu.roll(part, slots * p, 1))
        extra.append(jnp.broadcast_to(line[:, None, :], (askers, 8, LANES)))
    total = n_slots * 4
    extra = jnp.stack(extra, axis=1).reshape(total, LANES)
    extra = jnp.where(iota((total, LANES), 0) % 8 == 6, extra, 0.0)
    spread = jnp.broadcast_to((own.astype(I32) % 8)[:, None, :], (askers, capacity, LANES))
    spread = spread.reshape(total, LANES).astype(F32)
    place = iota((total, LANES), 0) % capacity
    keep = iota((total, LANES), 1) == (place // 8) * 2 + place % 2
    column = jnp.sum(jnp.where(keep, spread, 0.0), axis=1, keepdims=True)
    pltpu.make_async_copy(table_hbm.at[pl.ds(0, n_slots * 8), :], groups, sems.at[1]).wait()
    size = 32
    width = out_ref.shape[2]
    emb = groups.shape[1]
    r, c = iota((4 * size, 8 * size), 0), iota((4 * size, 8 * size), 1)
    offset = (c - 8 * (2 * (r // 8) + r % 2)).astype(F32)
    part_of = (r % 8) // 2
    for b in range(n_slots // size):
        rows = slice(b * 4 * size, (b + 1) * 4 * size)
        pick = jnp.where(offset == column[rows], 1.0, 0.0)
        blocks = []
        for q in range(4):
            chosen = jnp.where(part_of == q, pick, 0.0).astype(BF16)
            end = min(emb, (q + 1) * width)
            blocks.append(mm(chosen, groups[b * 8 * size : (b + 1) * 8 * size, q * width : end]))
        full = blocks[0] + blocks[1] + blocks[2]
        whole_part = jnp.concatenate(
            [full[:, :LANES] + blocks[3], full[:, LANES : 2 * LANES] + extra[rows], full[:, 2 * LANES :]],
            axis=1,
        )
        out_ref[b * size // 2 : (b + 1) * size // 2] = whole_part.astype(BF16).reshape(
            size // 2, 8, width
        )


def attention_kernel(
    lens_ref, z_ref, ids_ref, x_ref, qw_hbm, kvw_hbm, key_hbm, val_hbm, ow_hbm,
    out_ref, map_ref, qw, kvw, key, val, ow, sems, *, mapping,
):
    seqs, width = x_ref.shape
    ctx_len = key_hbm.shape[1]
    heads = qw_hbm.shape[1] // HEAD_DIM
    pad = 8
    copies = [
        pltpu.make_async_copy(src, dst, sems.at[i])
        for i, (src, dst) in enumerate(
            (
                (qw_hbm, qw),
                (kvw_hbm, kvw),
                (key_hbm, key),
                (val_hbm, val),
                (ow_hbm, ow),
            )
        )
    ]
    for copy in copies:
        copy.start()
    slot_map_kernel(z_ref, ids_ref, map_ref, **mapping)
    x = x_ref[...]
    copies[0].wait()
    query = mm(x, qw[...]).astype(BF16)
    src, dst = iota((HEAD_DIM, 4 * HEAD_DIM), 0), iota((HEAD_DIM, 4 * HEAD_DIM), 1)
    spread = ones_where(dst - jnp.where(dst < 2 * HEAD_DIM, 0, 2 * HEAD_DIM + 1) == 2 * src)
    blocks = width // HEAD_DIM
    stacked = jnp.concatenate(
        [x[:, g * HEAD_DIM : (g + 1) * HEAD_DIM] for g in range(blocks)], axis=0
    )
    wide = mm(stacked, spread).astype(BF16)
    even = jnp.concatenate(
        [wide[g * seqs : (g + 1) * seqs, : 2 * HEAD_DIM] for g in range(blocks)], axis=1
    )
    odd = jnp.concatenate(
        [wide[g * seqs : (g + 1) * seqs, 2 * HEAD_DIM :] for g in range(blocks)], axis=1
    )
    copies[1].wait()
    new_kv = mm(jnp.concatenate([even, odd], axis=0), kvw[...]).astype(BF16)
    rows = seqs * pad
    r, c = iota((rows, seqs), 0), iota((rows, seqs), 1)
    q_rows = jnp.zeros((rows, HEAD_DIM), F32)
    for g in range(heads):
        put = ones_where((r // pad == c) & (r % pad == g))
        q_rows = q_rows + mm(put, query[:, g * HEAD_DIM : (g + 1) * HEAD_DIM])
    rep = ones_where(r // pad == c)
    new_key = mm(rep, new_kv[:seqs, :])
    new_value = mm(rep, new_kv[seqs:, :])
    inv_scale = 1.0 / math.sqrt(HEAD_DIM)
    own = jnp.sum(q_rows * new_key, axis=1, keepdims=True) * inv_scale
    copies[2].wait()
    place = iota((pad, ctx_len), 1)
    energies = []
    for s in range(seqs):
        q_s = q_rows[s * pad : (s + 1) * pad, :].astype(BF16)
        score = mm_nt(q_s, key[s]) * inv_scale
        energies.append(jnp.where(place < lens_ref[s], score, -1e30))
    energies = jnp.concatenate(energies, axis=0)
    top = jnp.maximum(jnp.max(energies, axis=1, keepdims=True), own)
    weights = jnp.exp(energies - top)
    own_weight = jnp.exp(own - top)
    denom = jnp.sum(weights, axis=1, keepdims=True) + own_weight
    probs = weights / denom
    own_prob = (own_weight / denom).astype(BF16).astype(F32)
    copies[3].wait()
    context = []
    for s in range(seqs):
        context.append(mm(probs[s * pad : (s + 1) * pad, :].astype(BF16), val[s]))
    context = (jnp.concatenate(context, axis=0) + own_prob * new_value).astype(BF16)
    r, c = iota((seqs, rows), 0), iota((seqs, rows), 1)
    flat = []
    for g in range(heads):
        take = ones_where((c // pad == r) & (c % pad == g))
        flat.append(mm(take, context).astype(BF16))
    copies[4].wait()
    out_ref[...] = mm(jnp.concatenate(flat, axis=1), ow[...]).astype(BF16)


def mix_kernel(got_ref, map_ref, u_ref, more_u_ref, attn_ref, out_ref, *, width):
    total, columns = map_ref.shape
    seqs, emb = u_ref.shape
    part = got_ref.shape[2]
    rows = got_ref[...].reshape(total, part)
    of_seq = map_ref[...].astype(F32)
    u = u_ref[...].astype(F32) + more_u_ref[...].astype(F32)
    parts = columns // seqs
    u = jnp.concatenate([u, jnp.zeros((seqs, parts * part - emb), F32)], axis=1)
    u = jnp.concatenate([u[:, q * part : (q + 1) * part] for q in range(parts)], axis=0)
    u_high, u_low = two_parts(u)
    cross_all = (mm_nt(rows, u_high) + mm_nt(rows, u_low)) * of_seq
    r, c = iota((LANES, LANES), 0), iota((LANES, LANES), 1)
    same = ones_where((r // 8 == c // 8) & (r % 2 == c % 2))
    sums = []
    for b in range(0, total, LANES):
        high, mid, low = three_parts(cross_all[b : b + LANES, :])
        sums.append(mm(same, high) + (mm(same, mid) + mm(same, low)))
    cross = jnp.sum(jnp.concatenate(sums, axis=0), axis=1, keepdims=True)
    owners = total // 32
    row = iota((total, LANES), 0)
    extra = jnp.where(row % 8 == 6, rows[:, LANES : 2 * LANES].astype(F32), 0.0)
    extra = jnp.sum(extra.reshape(owners, 32, LANES), axis=1)
    square = extra + (pltpu.roll(extra, LANES - 8, 1) + pltpu.roll(extra, LANES - 16, 1))
    spread = jnp.broadcast_to(square[:, None, :], (owners, 32, LANES)).reshape(total, LANES)
    place = row % 32
    keep = iota((total, LANES), 1) == (place // 8) * 2 + place % 2
    square = jnp.sum(jnp.where(keep, spread, 0.0), axis=1, keepdims=True)
    gate = jax.nn.sigmoid(cross * lax.rsqrt(square / width + EPS) / math.sqrt(width))
    g_high, g_low = two_parts(of_seq * gate)
    mixed = mm_tn(g_high, rows) + mm_tn(g_low, rows)
    mixed = jnp.concatenate([mixed[q * seqs : (q + 1) * seqs, :] for q in range(parts)], axis=1)
    mixed = mixed[:, :emb].astype(BF16)
    peers = out_ref.shape[0]
    own = width // peers
    for p in range(peers):
        out_ref[p, :, :own] = attn_ref[:, p * own : (p + 1) * own]
        out_ref[p, :, own:] = mixed


def fetch_kernel(value_hbm, hidden_hbm, order_ref, value_ref, hidden_ref, sems):
    del order_ref
    copies = [
        pltpu.make_async_copy(value_hbm, value_ref, sems.at[0]),
        pltpu.make_async_copy(hidden_hbm, hidden_ref, sems.at[1]),
    ]
    for copy in copies:
        copy.start()
    for copy in copies:
        copy.wait()


def final_kernel(z_ref, got_ref, value_ref, hidden_ref, out_ref):
    part = out_ref.shape[1]
    first = pl.multiple_of(z_ref[0] * part, LANES)
    total = got_ref[0].astype(F32)
    for p in range(1, got_ref.shape[0]):
        total = total + got_ref[p].astype(F32)
    high, low = two_parts(total[:, part:])
    memory = mm(high, value_ref[...]) + mm(low, value_ref[...])
    out_ref[...] = (hidden_ref[:, pl.ds(first, part)].astype(F32) + total[:, :part] + memory).astype(BF16)


def body(
    hidden,
    attn_gain,
    q_weight,
    kv_weight,
    out_weight,
    key_cache,
    value_cache,
    cache_lengths,
    table,
    key_proj,
    value_proj,
    lookup_ids,
):
    seqs, width = hidden.shape
    lookups = lookup_ids.shape[1]
    requests = seqs * lookups
    rows_dev, emb = table.shape
    owners = lax.axis_size("table")
    tensor = lax.axis_size("tensor")
    me_table, me_tensor = lax.axis_index("table"), lax.axis_index("tensor")
    part = width // tensor
    capacity = 2 * requests // owners
    slots = capacity // tensor
    n_slots = owners * slots
    per = requests // LANES

    vmem = pl.BlockSpec(memory_space=pltpu.VMEM)
    smem = pl.BlockSpec(memory_space=pltpu.SMEM)
    hbm = pl.BlockSpec(memory_space=pl.ANY)
    ids_t = lookup_ids.T

    send = pl.pallas_call(
        send_ids_kernel,
        out_shape=jax.ShapeDtypeStruct((owners, per, LANES), I32),
        name="send_ids",
    )(ids_t)
    got_ids = lax.all_to_all(send, "table", 0, 0, tiled=True)

    def near(x):
        return pltpu.with_memory_space_constraint(x, pltpu.VMEM)

    me = me_table.astype(I32).reshape(1)
    z = me_tensor.astype(I32).reshape(1)
    chunks = (256, 256, 512, 1024, 1024, 1024)
    squares, u, attn_in = pl.pallas_call(
        lambda *refs: squares_kernel(*refs, chunks=chunks),
        in_specs=[smem, vmem, hbm, hbm, hbm, hbm],
        out_specs=[vmem, vmem, vmem],
        out_shape=[
            pltpu.VMEM((rows_dev // LANES, LANES), F32),
            jax.ShapeDtypeStruct((seqs, emb), BF16),
            jax.ShapeDtypeStruct(hidden.shape, BF16),
        ],
        scratch_shapes=[
            pltpu.VMEM(hidden.shape, BF16),
            pltpu.VMEM(key_proj.shape, BF16),
            pltpu.VMEM(table.shape, BF16),
            pltpu.VMEM((part, emb), BF16),
            pltpu.SemaphoreType.DMA((len(chunks) + 2,)),
        ],
        name="squares",
    )(z, attn_gain, hidden, key_proj, table, send)

    def other(x, step):
        return lax.ppermute(x, "tensor", [(i, i ^ step) for i in range(tensor)])

    more_u = other(u, 1)
    packed = pl.pallas_call(
        lambda *refs: gather_kernel(
            *refs, rows_dev=rows_dev, per=per, capacity=capacity, tensor=tensor
        ),
        in_specs=[smem, smem, vmem, vmem, hbm],
        out_specs=vmem,
        out_shape=jax.ShapeDtypeStruct((owners * tensor, 8, 3 * LANES), BF16),
        scratch_shapes=[
            pltpu.VMEM((n_slots // LANES, LANES), I32),
            pltpu.SMEM((n_slots // LANES, LANES), I32),
            pltpu.VMEM((n_slots * 8, emb), BF16),
            pltpu.SemaphoreType.DMA((2,)),
        ],
        name="gather",
    )(me, z, near(got_ids.reshape(owners * per, LANES)), near(squares), table)
    got_rows = lax.all_to_all(packed, ("table", "tensor"), 0, 0, tiled=True)
    u = (u.astype(F32) + more_u.astype(F32)).astype(BF16)
    more_u = other(u, 2)

    _, kv_width = key_cache.shape[1:]
    mapping = dict(rows_dev=rows_dev, owners=owners, seqs=seqs, lookups=lookups, capacity=capacity, tensor=tensor)
    attention, slot_map = pl.pallas_call(
        lambda *refs: attention_kernel(*refs, mapping=mapping),
        in_specs=[smem, smem, vmem, vmem, hbm, hbm, hbm, hbm, hbm],
        out_specs=[vmem, vmem],
        out_shape=[
            pltpu.VMEM((seqs, width), BF16),
            pltpu.VMEM((4 * n_slots, 4 * seqs), BF16),
        ],
        scratch_shapes=[
            pltpu.VMEM(q_weight.shape, BF16),
            pltpu.VMEM((2 * width, kv_width), BF16),
            pltpu.VMEM(key_cache.shape, BF16),
            pltpu.VMEM(value_cache.shape, BF16),
            pltpu.VMEM(out_weight.shape, BF16),
            pltpu.SemaphoreType.DMA((5,)),
        ],
        name="attention",
    )(
        cache_lengths, z, ids_t, attn_in, q_weight,
        kv_weight.reshape(2 * width, kv_width), key_cache, value_cache, out_weight,
    )

    mixes = pl.pallas_call(
        lambda *refs: mix_kernel(*refs, width=width),
        in_specs=[vmem] * 5,
        out_specs=vmem,
        out_shape=jax.ShapeDtypeStruct((tensor, seqs, part + emb), BF16),
        name="mix",
    )(near(got_rows), near(slot_map), near(u), near(more_u), near(attention))
    got_mixes = lax.all_to_all(mixes, "tensor", 0, 0, tiled=True)

    value_near, hidden_near = pl.pallas_call(
        fetch_kernel,
        in_specs=[hbm] * 3,
        out_specs=[vmem] * 2,
        out_shape=[pltpu.VMEM(value_proj.shape, BF16), pltpu.VMEM(hidden.shape, BF16)],
        scratch_shapes=[pltpu.SemaphoreType.DMA((2,))],
        name="fetch_value",
    )(value_proj, hidden, mixes)

    return pl.pallas_call(
        final_kernel,
        in_specs=[smem] + [vmem] * 3,
        out_specs=vmem,
        out_shape=jax.ShapeDtypeStruct((seqs, part), BF16),
        name="final",
    )(z, near(got_mixes), near(value_near), near(hidden_near))


def solution(mesh):
    return jax.shard_map(
        body,
        mesh=mesh,
        in_specs=(
            P("table", None),
            P(),
            P(None, "tensor"),
            P(None, None, "tensor"),
            P("tensor", None),
            P("table", None, "tensor"),
            P("table", None, "tensor"),
            P("table"),
            P("table", None),
            P(None, "tensor"),
            P(None, "tensor"),
            P("table", None),
        ),
        out_specs=P("table", "tensor"),
        check_vma=False,
    )
```

```python
import math

import jax
import jax.numpy as jnp
from jax import lax
from jax.experimental import pallas as pl
from jax.experimental.pallas import tpu as pltpu
from jax.sharding import PartitionSpec as P


HEAD_DIM = 128
EPS = 1e-06
LANES = 128
F32 = jnp.float32
BF16 = jnp.bfloat16
I32 = jnp.int32


def iota(shape, dim):
    return lax.broadcasted_iota(I32, shape, dim)


def ones_where(mask):
    return jnp.where(mask, 1.0, 0.0).astype(BF16)


def mm(a, b):
    return lax.dot_general(a, b, (((1,), (0,)), ((), ())), preferred_element_type=F32)


def mm_nt(a, b):
    return lax.dot_general(a, b, (((1,), (1,)), ((), ())), preferred_element_type=F32)


def mm_tn(a, b):
    return lax.dot_general(a, b, (((0,), (0,)), ((), ())), preferred_element_type=F32)


def two_parts(x):
    high = x.astype(BF16)
    return high, (x - high.astype(F32)).astype(BF16)


def three_parts(x):
    high = x.astype(BF16)
    rest = x - high.astype(F32)
    mid = rest.astype(BF16)
    return high, mid, (rest - mid.astype(F32)).astype(BF16)


def start_kernel(
    ids_hbm, gain_hbm, hidden_hbm, key_hbm, send_hbm, u_ref, attn_in_ref, key_t,
    ids_ref, gain_ref, hidden_ref, key_ref, send_ref, sems,
):
    copies = [
        pltpu.make_async_copy(src, dst, sems.at[i])
        for i, (src, dst) in enumerate(
            ((ids_hbm, ids_ref), (hidden_hbm, hidden_ref), (gain_hbm, gain_ref), (key_hbm, key_ref))
        )
    ]
    for copy in copies:
        copy.start()
    _, per, _ = send_ref.shape
    _, seqs = ids_ref.shape
    fit = LANES // seqs
    copies[0].wait()
    flat = [
        jnp.concatenate([ids_ref[j * fit + q : j * fit + q + 1, :] for q in range(fit)], axis=1)
        for j in range(per)
    ]
    send_ref[...] = jnp.broadcast_to(jnp.concatenate(flat, axis=0)[None], send_ref.shape)
    out = pltpu.make_async_copy(send_ref, send_hbm, sems.at[4])
    out.start()
    copies[1].wait()
    part = key_ref.shape[1]
    hidden = hidden_ref[...].astype(F32)
    inv = lax.rsqrt(jnp.mean(hidden * hidden, axis=1, keepdims=True) + EPS)
    copies[2].wait()
    attn_in_ref[...] = (hidden * inv * gain_ref[...].reshape(1, hidden.shape[1])).astype(BF16)
    first = pl.multiple_of(lax.axis_index("tensor") * part, LANES)
    high, low = two_parts(hidden_ref[:, pl.ds(first, part)].astype(F32) * inv)
    copies[3].wait()
    key_t[...] = key_ref[...].T
    u = mm(jnp.concatenate([high, low], axis=0), key_t[...])
    u_ref[...] = (u[:seqs] + u[seqs:]).astype(BF16)
    out.wait()


def slot_map_kernel(ids_ref, map_ref, *, rows_dev, owners, seqs, lookups, capacity, tensor):
    requests = seqs * lookups
    total, width = map_ref.shape
    ids = jnp.concatenate([ids_ref[j : j + 1, :] for j in range(lookups)], axis=1)
    owner = ids // rows_dev
    hit = ones_where(iota((owners, requests), 0) == owner)
    before = ones_where(iota((requests, requests), 0) < iota((requests, requests), 1))
    rank = jnp.sum(mm(hit, before) * hit.astype(F32), axis=0, keepdims=True).astype(I32)
    key = owner * capacity + rank - lax.axis_index("tensor") * (capacity // tensor)
    row = iota((total, requests), 0)
    place = row % capacity
    placed = ones_where(row - place + (place // 8) * 2 + place % 2 == key)
    of_seq = ones_where(iota((width, requests), 1) % seqs == iota((width, requests), 0) % seqs)
    part = (iota((total, width), 0) % 8) // 2
    known = mm_nt(placed, of_seq)
    map_ref[...] = jnp.where(part == iota((total, width), 1) // seqs, known, 0.0).astype(BF16)


def fetch_rows(table_hbm, table, sems, first, chunks):
    copies, start = [], 0
    for i, size in enumerate(chunks):
        copies.append(
            pltpu.make_async_copy(
                table_hbm.at[pl.ds(first + start, size), :],
                table.at[pl.ds(start, size), :],
                sems.at[i],
            )
        )
        copies[-1].start()
        start += size
    return copies


def row_squares(key_t, table, squares, copies, first, chunks, between=None):
    sub, start = 256, 0
    for copy, size in zip(copies, chunks):
        copy.wait()
        for t in range(start, start + size, sub):
            if between is not None and t == 0:
                for i in range(sum(chunks) // sub):
                    between(i)
            keys = mm_nt(key_t[...], table[t : t + sub, :])
            line = jnp.sum(keys * keys, axis=0, keepdims=True)
            for g in range(sub // LANES):
                group = (first + t) // LANES + g
                squares[group : group + 1, :] = line[:, g * LANES : (g + 1) * LANES]
        start += size


def squares_kernel(key_t, table_hbm, squares, table, sems, *, chunks):
    row_squares(key_t, table, squares, fetch_rows(table_hbm, table, sems, 0, chunks), 0, chunks)


def slot_lanes(row, z, slots):
    askers = row.shape[0]
    lane = iota((askers, LANES), 1)
    own = row if z == 0 else pltpu.roll(row, LANES - z * slots, 1)
    own = jnp.where(lane < slots, own, 0.0)
    step = slots
    while step < LANES:
        own = own + pltpu.roll(own, step, 1)
        step *= 2
    fit = LANES // slots
    own = jnp.where(lane // slots == iota((askers, LANES), 0) % fit, own, 0.0)
    return jnp.sum(own.reshape(askers // fit, fit, LANES), axis=1)


def gather_kernel(
    got_ref, some_ref, key_t, table_hbm, out_hbm,
    idx_vmem, idx_smem, groups, out_ref, table, sq_ref, sems, table_sems,
    *, rows_dev, per, capacity, tensor, chunks,
):
    askers = got_ref.shape[0] // per
    slots = capacity // tensor
    n_slots = askers * slots
    me, mine_z = lax.axis_index("table"), lax.axis_index("tensor")
    done = some_ref.shape[0]
    copies = fetch_rows(table_hbm, table, table_sems, done * LANES, chunks)
    sq_ref[:done, :] = some_ref[...]
    before = ones_where(iota((LANES, LANES), 0) < iota((LANES, LANES), 1))
    lane = iota((askers, LANES), 1)
    seen = jnp.zeros((askers, 1), F32)
    ranks, locals_ = [], []
    for j in range(per):
        local = got_ref[pl.ds(j, askers, stride=per), :] - me * rows_dev
        mine = (local >= 0) & (local < rows_dev)
        rank = mm(ones_where(mine), before) + seen
        seen = seen + jnp.sum(jnp.where(mine, 1.0, 0.0), axis=1, keepdims=True)
        ranks.append(jnp.where(mine, rank, -1.0).astype(I32))
        locals_.append(local.astype(F32))

    def ranked(target):
        one = jnp.where(ranks[0] == target, locals_[0], 0.0)
        for j in range(1, per):
            one = one + jnp.where(ranks[j] == target, locals_[j], 0.0)
        return jnp.sum(one, axis=1, keepdims=True)

    own = jnp.zeros((askers, LANES), F32)
    for k in range(slots):
        own = jnp.where(lane == k, ranked((k // 2) * slots + k % 2 + 2 * mine_z), own)
    idx_vmem[...] = slot_lanes(own, 0, slots).astype(I32)
    to_smem = pltpu.make_async_copy(idx_vmem, idx_smem, sems.at[0])
    to_smem.start()
    row = jnp.zeros((askers, LANES), F32)
    for k in range(capacity):
        row = jnp.where(lane == k, ranked(k), row)
    to_smem.wait()
    half = n_slots // 2
    steps = sum(chunks) // 256
    each = n_slots // steps

    def issue(step):
        for s in range(step * each, (step + 1) * each):
            base = pl.multiple_of((idx_smem[s // LANES, s % LANES] // 8) * 8, 8)
            pltpu.make_async_copy(
                table_hbm.at[pl.ds(base, 8), :],
                groups.at[pl.ds(s * 8, 8), :],
                sems.at[1 + s // half],
            ).start()

    row_squares(key_t, table, sq_ref, copies, done * LANES, chunks, issue)
    ids = row.astype(I32)
    high, low = ids // LANES, ids % LANES
    value = jnp.zeros((askers, LANES), F32)
    for g in range(sq_ref.shape[0]):
        line = jnp.broadcast_to(sq_ref[g : g + 1, :], (askers, LANES))
        found = jnp.take_along_axis(line, low, axis=1, mode="promise_in_bounds")
        value = jnp.where(high == g, found, value)
    extra = []
    for z in range(tensor):
        piece = value if z == 0 else pltpu.roll(value, LANES - slots * z, 1)
        line = jnp.zeros((askers, LANES), F32)
        for p, part in enumerate(three_parts(jnp.where(lane < slots, piece, 0.0))):
            part = part.astype(F32)
            line = line + (part if p == 0 else pltpu.roll(part, slots * p, 1))
        extra.append(line.astype(BF16))
    extra = jnp.concatenate(extra, axis=0)
    spread = jnp.broadcast_to((own.astype(I32) % 8)[:, None, :], (askers, slots, LANES))
    spread = spread.reshape(n_slots, LANES).astype(F32)
    keep = iota((n_slots, LANES), 1) == iota((n_slots, LANES), 0) % slots
    column = jnp.sum(jnp.where(keep, spread, 0.0), axis=1, keepdims=True)
    size = 32
    width = out_ref.shape[2]
    emb = groups.shape[1]
    offset = (iota((size, 8 * size), 1) - 8 * iota((size, 8 * size), 0)).astype(F32)
    r, c = iota((4 * size, size), 0), iota((4 * size, size), 1)
    move = [ones_where((c == 2 * (r // 8) + r % 2) & ((r % 8) // 2 == q)) for q in range(4)]
    r, c = iota((4 * size, LANES), 0), iota((4 * size, LANES), 1)
    source = jnp.where(r % 8 == 6, ((r // 8) % tensor) * askers + r // capacity, -LANES)
    blocks = n_slots // size
    outs = []
    for b in range(blocks):
        if b % (blocks // 2) == 0:
            h = b // (blocks // 2)
            pltpu.make_async_copy(
                table_hbm.at[pl.ds(0, half * 8), :],
                groups.at[pl.ds(h * half * 8, half * 8), :],
                sems.at[1 + h],
            ).wait()
        pick = ones_where(offset == column[b * size : (b + 1) * size, :])
        rows = mm(pick, groups[b * 8 * size : (b + 1) * 8 * size, :]).astype(BF16)
        full = mm(move[0], rows[:, :width])
        for q in (1, 2):
            full = full + mm(move[q], rows[:, q * width : (q + 1) * width])
        tail = mm(move[3], rows[:, 3 * width : emb])
        squares = mm(ones_where(c == source + b * (size // slots)), extra)
        full = jnp.concatenate(
            [full[:, :LANES] + tail, full[:, LANES : 2 * LANES] + squares, full[:, 2 * LANES :]],
            axis=1,
        )
        span = pl.ds(b * size // 2, size // 2)
        out_ref[b * size // 2 : (b + 1) * size // 2] = full.astype(BF16).reshape(size // 2, 8, width)
        outs.append(pltpu.make_async_copy(out_ref.at[span], out_hbm.at[span], sems.at[3 + b]))
        outs[-1].start()
    for out in outs:
        out.wait()


def attention_kernel(
    lens_ref, ids_ref, x_ref, qw_hbm, kvw_hbm, key_hbm, val_hbm, ow_hbm,
    out_ref, map_ref, qw, kvw, key, val, ow, sems, *, mapping,
):
    seqs, width = x_ref.shape
    ctx_len = key_hbm.shape[1]
    heads = qw_hbm.shape[1] // HEAD_DIM
    pad = 8
    copies = [
        pltpu.make_async_copy(src, dst, sems.at[i])
        for i, (src, dst) in enumerate(
            (
                (qw_hbm, qw),
                (kvw_hbm, kvw),
                (key_hbm, key),
                (val_hbm, val),
                (ow_hbm, ow),
            )
        )
    ]
    for copy in copies:
        copy.start()
    slot_map_kernel(ids_ref, map_ref, **mapping)
    x = x_ref[...]
    copies[0].wait()
    query = mm(x, qw[...]).astype(BF16)
    src, dst = iota((HEAD_DIM, 4 * HEAD_DIM), 0), iota((HEAD_DIM, 4 * HEAD_DIM), 1)
    spread = ones_where(dst - jnp.where(dst < 2 * HEAD_DIM, 0, 2 * HEAD_DIM + 1) == 2 * src)
    blocks = width // HEAD_DIM
    stacked = jnp.concatenate(
        [x[:, g * HEAD_DIM : (g + 1) * HEAD_DIM] for g in range(blocks)], axis=0
    )
    wide = mm(stacked, spread).astype(BF16)
    even = jnp.concatenate(
        [wide[g * seqs : (g + 1) * seqs, : 2 * HEAD_DIM] for g in range(blocks)], axis=1
    )
    odd = jnp.concatenate(
        [wide[g * seqs : (g + 1) * seqs, 2 * HEAD_DIM :] for g in range(blocks)], axis=1
    )
    copies[1].wait()
    new_kv = mm(jnp.concatenate([even, odd], axis=0), kvw[...]).astype(BF16)
    rows = seqs * pad
    r, c = iota((rows, seqs), 0), iota((rows, seqs), 1)
    q_rows = jnp.zeros((rows, HEAD_DIM), F32)
    for g in range(heads):
        put = ones_where((r // pad == c) & (r % pad == g))
        q_rows = q_rows + mm(put, query[:, g * HEAD_DIM : (g + 1) * HEAD_DIM])
    rep = ones_where(r // pad == c)
    new_key = mm(rep, new_kv[:seqs, :])
    new_value = mm(rep, new_kv[seqs:, :])
    inv_scale = 1.0 / math.sqrt(HEAD_DIM)
    own = jnp.sum(q_rows * new_key, axis=1, keepdims=True) * inv_scale
    copies[2].wait()
    place = iota((pad, ctx_len), 1)
    energies = []
    for s in range(seqs):
        q_s = q_rows[s * pad : (s + 1) * pad, :].astype(BF16)
        score = mm_nt(q_s, key[s]) * inv_scale
        energies.append(jnp.where(place < lens_ref[s], score, -1e30))
    energies = jnp.concatenate(energies, axis=0)
    top = jnp.maximum(jnp.max(energies, axis=1, keepdims=True), own)
    weights = jnp.exp(energies - top)
    own_weight = jnp.exp(own - top)
    denom = jnp.sum(weights, axis=1, keepdims=True) + own_weight
    probs = weights / denom
    own_prob = (own_weight / denom).astype(BF16).astype(F32)
    copies[3].wait()
    context = []
    for s in range(seqs):
        context.append(mm(probs[s * pad : (s + 1) * pad, :].astype(BF16), val[s]))
    context = (jnp.concatenate(context, axis=0) + own_prob * new_value).astype(BF16)
    r, c = iota((seqs, rows), 0), iota((seqs, rows), 1)
    flat = []
    for g in range(heads):
        take = ones_where((c // pad == r) & (c % pad == g))
        flat.append(mm(take, context).astype(BF16))
    copies[4].wait()
    out_ref[...] = mm(jnp.concatenate(flat, axis=1), ow[...]).astype(BF16)


def mix_kernel(got_ref, map_ref, u_ref, more_u_ref, attn_ref, out_ref, *, width):
    total, columns = map_ref.shape
    seqs, emb = u_ref.shape
    part = got_ref.shape[2]
    rows = got_ref[...].reshape(total, part)
    of_seq = map_ref[...].astype(F32)
    u = u_ref[...].astype(F32) + more_u_ref[...].astype(F32)
    parts = columns // seqs
    u = jnp.concatenate([u, jnp.zeros((seqs, parts * part - emb), F32)], axis=1)
    u = jnp.concatenate([u[:, q * part : (q + 1) * part] for q in range(parts)], axis=0)
    u_high, u_low = two_parts(u)
    cross_all = (mm_nt(rows, u_high) + mm_nt(rows, u_low)) * of_seq
    r, c = iota((LANES, LANES), 0), iota((LANES, LANES), 1)
    same = ones_where((r // 8 == c // 8) & (r % 2 == c % 2))
    sums = []
    for b in range(0, total, LANES):
        high, mid, low = three_parts(cross_all[b : b + LANES, :])
        sums.append(mm(same, high) + (mm(same, mid) + mm(same, low)))
    cross = jnp.sum(jnp.concatenate(sums, axis=0), axis=1, keepdims=True)
    owners = total // 32
    row = iota((total, LANES), 0)
    extra = jnp.where(row % 8 == 6, rows[:, LANES : 2 * LANES].astype(F32), 0.0)
    extra = jnp.sum(extra.reshape(owners, 32, LANES), axis=1)
    square = extra + (pltpu.roll(extra, LANES - 8, 1) + pltpu.roll(extra, LANES - 16, 1))
    spread = jnp.broadcast_to(square[:, None, :], (owners, 32, LANES)).reshape(total, LANES)
    place = row % 32
    keep = iota((total, LANES), 1) == (place // 8) * 2 + place % 2
    square = jnp.sum(jnp.where(keep, spread, 0.0), axis=1, keepdims=True)
    gate = jax.nn.sigmoid(cross * lax.rsqrt(square / width + EPS) / math.sqrt(width))
    g_high, g_low = two_parts(of_seq * gate)
    mixed = mm_tn(g_high, rows) + mm_tn(g_low, rows)
    mixed = jnp.concatenate([mixed[q * seqs : (q + 1) * seqs, :] for q in range(parts)], axis=1)
    mixed = mixed[:, :emb].astype(BF16)
    peers = out_ref.shape[0]
    own = width // peers
    for p in range(peers):
        out_ref[p, :, :own] = attn_ref[:, p * own : (p + 1) * own]
        out_ref[p, :, own:] = mixed


def fetch_kernel(value_hbm, hidden_hbm, order_ref, value_ref, hidden_ref, sems):
    del order_ref
    copies = [
        pltpu.make_async_copy(value_hbm, value_ref, sems.at[0]),
        pltpu.make_async_copy(hidden_hbm, hidden_ref, sems.at[1]),
    ]
    for copy in copies:
        copy.start()
    for copy in copies:
        copy.wait()


def final_kernel(got_ref, value_ref, hidden_ref, out_ref):
    part = out_ref.shape[1]
    first = pl.multiple_of(lax.axis_index("tensor") * part, LANES)
    total = got_ref[0].astype(F32)
    for p in range(1, got_ref.shape[0]):
        total = total + got_ref[p].astype(F32)
    high, low = two_parts(total[:, part:])
    memory = mm(high, value_ref[...]) + mm(low, value_ref[...])
    out_ref[...] = (hidden_ref[:, pl.ds(first, part)].astype(F32) + total[:, :part] + memory).astype(BF16)


def body(
    hidden,
    attn_gain,
    q_weight,
    kv_weight,
    out_weight,
    key_cache,
    value_cache,
    cache_lengths,
    table,
    key_proj,
    value_proj,
    lookup_ids,
):
    seqs, width = hidden.shape
    lookups = lookup_ids.shape[1]
    requests = seqs * lookups
    rows_dev, emb = table.shape
    owners = lax.axis_size("table")
    tensor = lax.axis_size("tensor")
    part = width // tensor
    capacity = 2 * requests // owners
    slots = capacity // tensor
    n_slots = owners * slots
    per = requests // LANES

    vmem = pl.BlockSpec(memory_space=pltpu.VMEM)
    smem = pl.BlockSpec(memory_space=pltpu.SMEM)
    hbm = pl.BlockSpec(memory_space=pl.ANY)
    ids_t = lookup_ids.T

    def near(x):
        return pltpu.with_memory_space_constraint(x, pltpu.VMEM)

    def other(x, step):
        return lax.ppermute(x, "tensor", [(i, i ^ step) for i in range(tensor)])

    send, u, attn_in, key_t = pl.pallas_call(
        start_kernel,
        in_specs=[hbm] * 4,
        out_specs=[hbm] + [vmem] * 3,
        out_shape=[
            jax.ShapeDtypeStruct((owners, per, LANES), I32),
            pltpu.VMEM((seqs, emb), BF16),
            pltpu.VMEM(hidden.shape, BF16),
            pltpu.VMEM((part, emb), BF16),
        ],
        scratch_shapes=[
            pltpu.VMEM(ids_t.shape, I32),
            pltpu.VMEM(attn_gain.shape, F32),
            pltpu.VMEM(hidden.shape, BF16),
            pltpu.VMEM(key_proj.shape, BF16),
            pltpu.VMEM((owners, per, LANES), I32),
            pltpu.SemaphoreType.DMA((5,)),
        ],
        name="start",
    )(ids_t, attn_gain, hidden, key_proj)
    more_u = other(u, 1)
    got_ids = lax.all_to_all(send, "table", 0, 0, tiled=True)

    u = (u.astype(F32) + more_u.astype(F32)).astype(BF16)
    more_u = other(u, 2)

    chunks = (256, 256, 512, 1024)
    more_chunks = (1024, 1024)
    early_rows = sum(chunks)
    squares = pl.pallas_call(
        lambda *refs: squares_kernel(*refs, chunks=chunks),
        in_specs=[vmem, hbm],
        out_specs=vmem,
        out_shape=pltpu.VMEM((early_rows // LANES, LANES), F32),
        scratch_shapes=[
            pltpu.VMEM((early_rows, emb), BF16),
            pltpu.SemaphoreType.DMA((len(chunks),)),
        ],
        name="squares",
    )(near(key_t), table)

    packed = pl.pallas_call(
        lambda *refs: gather_kernel(
            *refs, rows_dev=rows_dev, per=per, capacity=capacity, tensor=tensor, chunks=more_chunks
        ),
        in_specs=[vmem, vmem, vmem, hbm],
        out_specs=hbm,
        out_shape=jax.ShapeDtypeStruct((owners * tensor, 8, 3 * LANES), BF16),
        scratch_shapes=[
            pltpu.VMEM((n_slots // LANES, LANES), I32),
            pltpu.SMEM((n_slots // LANES, LANES), I32),
            pltpu.VMEM((n_slots * 8, emb), BF16),
            pltpu.VMEM((owners * tensor, 8, 3 * LANES), BF16),
            pltpu.VMEM((rows_dev - early_rows, emb), BF16),
            pltpu.VMEM((rows_dev // LANES, LANES), F32),
            pltpu.SemaphoreType.DMA((11,)),
            pltpu.SemaphoreType.DMA((len(more_chunks),)),
        ],
        name="gather",
    )(near(got_ids.reshape(owners * per, LANES)), near(squares), near(key_t), table)
    got_rows = lax.all_to_all(packed, ("table", "tensor"), 0, 0, tiled=True)
    _, kv_width = key_cache.shape[1:]
    mapping = dict(rows_dev=rows_dev, owners=owners, seqs=seqs, lookups=lookups, capacity=capacity, tensor=tensor)
    attention, slot_map = pl.pallas_call(
        lambda *refs: attention_kernel(*refs, mapping=mapping),
        in_specs=[smem, vmem, vmem, hbm, hbm, hbm, hbm, hbm],
        out_specs=[vmem, vmem],
        out_shape=[
            pltpu.VMEM((seqs, width), BF16),
            pltpu.VMEM((4 * n_slots, 4 * seqs), BF16),
        ],
        scratch_shapes=[
            pltpu.VMEM(q_weight.shape, BF16),
            pltpu.VMEM((2 * width, kv_width), BF16),
            pltpu.VMEM(key_cache.shape, BF16),
            pltpu.VMEM(value_cache.shape, BF16),
            pltpu.VMEM(out_weight.shape, BF16),
            pltpu.SemaphoreType.DMA((5,)),
        ],
        name="attention",
    )(
        cache_lengths, ids_t, near(attn_in), q_weight,
        kv_weight.reshape(2 * width, kv_width), key_cache, value_cache, out_weight,
    )

    mixes = pl.pallas_call(
        lambda *refs: mix_kernel(*refs, width=width),
        in_specs=[vmem] * 5,
        out_specs=vmem,
        out_shape=jax.ShapeDtypeStruct((tensor, seqs, part + emb), BF16),
        name="mix",
    )(near(got_rows), near(slot_map), near(u), near(more_u), near(attention))
    got_mixes = lax.all_to_all(mixes, "tensor", 0, 0, tiled=True)

    value_near, hidden_near = pl.pallas_call(
        fetch_kernel,
        in_specs=[hbm] * 3,
        out_specs=[vmem] * 2,
        out_shape=[pltpu.VMEM(value_proj.shape, BF16), pltpu.VMEM(hidden.shape, BF16)],
        scratch_shapes=[pltpu.SemaphoreType.DMA((2,))],
        name="fetch_value",
    )(value_proj, hidden, mixes)

    return pl.pallas_call(
        final_kernel,
        in_specs=[vmem] * 3,
        out_specs=vmem,
        out_shape=jax.ShapeDtypeStruct((seqs, part), BF16),
        name="final",
    )(near(got_mixes), near(value_near), near(hidden_near))


def solution(mesh):
    return jax.shard_map(
        body,
        mesh=mesh,
        in_specs=(
            P("table", None),
            P(),
            P(None, "tensor"),
            P(None, None, "tensor"),
            P("tensor", None),
            P("table", None, "tensor"),
            P("table", None, "tensor"),
            P("table"),
            P("table", None),
            P(None, "tensor"),
            P(None, "tensor"),
            P("table", None),
        ),
        out_specs=P("table", "tensor"),
        check_vma=False,
    )
```

```python
import math

import jax
import jax.numpy as jnp
from jax import lax
from jax.experimental import pallas as pl
from jax.experimental.pallas import tpu as pltpu
from jax.sharding import PartitionSpec as P


HEAD_DIM = 128
EPS = 1e-06
LANES = 128
F32 = jnp.float32
BF16 = jnp.bfloat16
I32 = jnp.int32


def iota(shape, dim):
    return lax.broadcasted_iota(I32, shape, dim)


def ones_where(mask):
    return jnp.where(mask, 1.0, 0.0).astype(BF16)


def mm(a, b):
    return lax.dot_general(a, b, (((1,), (0,)), ((), ())), preferred_element_type=F32)


def mm_nt(a, b):
    return lax.dot_general(a, b, (((1,), (1,)), ((), ())), preferred_element_type=F32)


def mm_tn(a, b):
    return lax.dot_general(a, b, (((0,), (0,)), ((), ())), preferred_element_type=F32)


def two_parts(x):
    high = x.astype(BF16)
    return high, (x - high.astype(F32)).astype(BF16)


def three_parts(x):
    high = x.astype(BF16)
    rest = x - high.astype(F32)
    mid = rest.astype(BF16)
    return high, mid, (rest - mid.astype(F32)).astype(BF16)


def start_kernel(
    ids_hbm, gain_hbm, hidden_hbm, key_hbm, send_hbm, u_ref, attn_in_ref, key_t,
    ids_ref, gain_ref, hidden_ref, key_ref, send_ref, sems,
):
    copies = [
        pltpu.make_async_copy(src, dst, sems.at[i])
        for i, (src, dst) in enumerate(
            ((ids_hbm, ids_ref), (hidden_hbm, hidden_ref), (gain_hbm, gain_ref), (key_hbm, key_ref))
        )
    ]
    for copy in copies:
        copy.start()
    _, per, _ = send_ref.shape
    _, seqs = ids_ref.shape
    fit = LANES // seqs
    copies[0].wait()
    flat = [
        jnp.concatenate([ids_ref[j * fit + q : j * fit + q + 1, :] for q in range(fit)], axis=1)
        for j in range(per)
    ]
    send_ref[...] = jnp.broadcast_to(jnp.concatenate(flat, axis=0)[None], send_ref.shape)
    out = pltpu.make_async_copy(send_ref, send_hbm, sems.at[4])
    out.start()
    copies[1].wait()
    part = key_ref.shape[1]
    hidden = hidden_ref[...].astype(F32)
    inv = lax.rsqrt(jnp.mean(hidden * hidden, axis=1, keepdims=True) + EPS)
    copies[2].wait()
    attn_in_ref[...] = (hidden * inv * gain_ref[...].reshape(1, hidden.shape[1])).astype(BF16)
    first = pl.multiple_of(lax.axis_index("tensor") * part, LANES)
    high, low = two_parts(hidden_ref[:, pl.ds(first, part)].astype(F32) * inv)
    copies[3].wait()
    key_t[...] = key_ref[...].T
    u = mm(jnp.concatenate([high, low], axis=0), key_t[...])
    u_ref[...] = (u[:seqs] + u[seqs:]).astype(BF16)
    out.wait()


def slot_map_kernel(ids_ref, map_ref, *, rows_dev, owners, seqs, lookups, capacity, tensor):
    requests = seqs * lookups
    total, width = map_ref.shape
    ids = jnp.concatenate([ids_ref[j : j + 1, :] for j in range(lookups)], axis=1)
    owner = ids // rows_dev
    hit = ones_where(iota((owners, requests), 0) == owner)
    before = ones_where(iota((requests, requests), 0) < iota((requests, requests), 1))
    rank = jnp.sum(mm(hit, before) * hit.astype(F32), axis=0, keepdims=True).astype(I32)
    key = owner * capacity + rank - lax.axis_index("tensor") * (capacity // tensor)
    row = iota((total, requests), 0)
    place = row % capacity
    placed = ones_where(row - place + (place // 8) * 2 + place % 2 == key)
    of_seq = ones_where(iota((width, requests), 1) % seqs == iota((width, requests), 0) % seqs)
    part = (iota((total, width), 0) % 8) // 2
    known = mm_nt(placed, of_seq)
    map_ref[...] = jnp.where(part == iota((total, width), 1) // seqs, known, 0.0).astype(BF16)


def fetch_rows(table_hbm, table, sems, first, chunks):
    copies, start = [], 0
    for i, size in enumerate(chunks):
        copies.append(
            pltpu.make_async_copy(
                table_hbm.at[pl.ds(first + start, size), :],
                table.at[pl.ds(start, size), :],
                sems.at[i],
            )
        )
        copies[-1].start()
        start += size
    return copies


def row_squares(key_t, table, squares, copies, first, chunks, between=None):
    sub, start = 256, 0
    for copy, size in zip(copies, chunks):
        copy.wait()
        for t in range(start, start + size, sub):
            if between is not None and t == 0:
                for i in range(sum(chunks) // sub):
                    between(i)
            keys = mm_nt(key_t[...], table[t : t + sub, :])
            line = jnp.sum(keys * keys, axis=0, keepdims=True)
            for g in range(sub // LANES):
                group = (first + t) // LANES + g
                squares[group : group + 1, :] = line[:, g * LANES : (g + 1) * LANES]
        start += size


def squares_kernel(key_t, table_hbm, squares, table, sems, *, chunks):
    row_squares(key_t, table, squares, fetch_rows(table_hbm, table, sems, 0, chunks), 0, chunks)


def slot_lanes(row, z, slots):
    askers = row.shape[0]
    lane = iota((askers, LANES), 1)
    own = row if z == 0 else pltpu.roll(row, LANES - z * slots, 1)
    own = jnp.where(lane < slots, own, 0.0)
    step = slots
    while step < LANES:
        own = own + pltpu.roll(own, step, 1)
        step *= 2
    fit = LANES // slots
    own = jnp.where(lane // slots == iota((askers, LANES), 0) % fit, own, 0.0)
    return jnp.sum(own.reshape(askers // fit, fit, LANES), axis=1)


def gather_kernel(
    got_ref, some_ref, key_t, table_hbm, out_hbm,
    idx_vmem, idx_smem, groups, out_ref, table, sq_ref, sems, table_sems,
    *, rows_dev, per, capacity, tensor, chunks,
):
    askers = got_ref.shape[0] // per
    slots = capacity // tensor
    n_slots = askers * slots
    me, mine_z = lax.axis_index("table"), lax.axis_index("tensor")
    done = some_ref.shape[0]
    copies = fetch_rows(table_hbm, table, table_sems, done * LANES, chunks)
    sq_ref[:done, :] = some_ref[...]
    before = ones_where(iota((LANES, LANES), 0) < iota((LANES, LANES), 1))
    lane = iota((askers, LANES), 1)
    seen = jnp.zeros((askers, 1), F32)
    ranks, locals_ = [], []
    for j in range(per):
        local = got_ref[pl.ds(j, askers, stride=per), :] - me * rows_dev
        mine = (local >= 0) & (local < rows_dev)
        rank = mm(ones_where(mine), before) + seen
        seen = seen + jnp.sum(jnp.where(mine, 1.0, 0.0), axis=1, keepdims=True)
        ranks.append(jnp.where(mine, rank, -1.0).astype(I32))
        locals_.append(local.astype(F32))

    def ranked(target):
        one = jnp.where(ranks[0] == target, locals_[0], 0.0)
        for j in range(1, per):
            one = one + jnp.where(ranks[j] == target, locals_[j], 0.0)
        return jnp.sum(one, axis=1, keepdims=True)

    own = jnp.zeros((askers, LANES), F32)
    for k in range(slots):
        own = jnp.where(lane == k, ranked((k // 2) * slots + k % 2 + 2 * mine_z), own)
    idx_vmem[...] = slot_lanes(own, 0, slots).astype(I32)
    to_smem = pltpu.make_async_copy(idx_vmem, idx_smem, sems.at[0])
    to_smem.start()
    row = jnp.zeros((askers, LANES), F32)
    for k in range(capacity):
        row = jnp.where(lane == k, ranked(k), row)
    to_smem.wait()
    half = n_slots // 2
    steps = sum(chunks) // 256
    each = n_slots // steps

    def issue(step):
        for s in range(step * each, (step + 1) * each):
            base = pl.multiple_of((idx_smem[s // LANES, s % LANES] // 2) * 2, 2)
            pltpu.make_async_copy(
                table_hbm.at[pl.ds(base, 2), :],
                groups.at[pl.ds(s * 2, 2), :],
                sems.at[1 + s // half],
            ).start()

    row_squares(key_t, table, sq_ref, copies, done * LANES, chunks, issue)
    ids = row.astype(I32)
    high, low = ids // LANES, ids % LANES
    value = jnp.zeros((askers, LANES), F32)
    for g in range(sq_ref.shape[0]):
        line = jnp.broadcast_to(sq_ref[g : g + 1, :], (askers, LANES))
        found = jnp.take_along_axis(line, low, axis=1, mode="promise_in_bounds")
        value = jnp.where(high == g, found, value)
    extra = []
    for z in range(tensor):
        piece = value if z == 0 else pltpu.roll(value, LANES - slots * z, 1)
        line = jnp.zeros((askers, LANES), F32)
        for p, part in enumerate(three_parts(jnp.where(lane < slots, piece, 0.0))):
            part = part.astype(F32)
            line = line + (part if p == 0 else pltpu.roll(part, slots * p, 1))
        extra.append(line.astype(BF16))
    extra = jnp.concatenate(extra, axis=0)
    spread = jnp.broadcast_to((own.astype(I32) % 2)[:, None, :], (askers, slots, LANES))
    spread = spread.reshape(n_slots, LANES).astype(F32)
    keep = iota((n_slots, LANES), 1) == iota((n_slots, LANES), 0) % slots
    column = jnp.sum(jnp.where(keep, spread, 0.0), axis=1, keepdims=True)
    size = 64
    width = out_ref.shape[2]
    emb = groups.shape[1]
    offset = (iota((size, 2 * size), 1) - 2 * iota((size, 2 * size), 0)).astype(F32)
    r, c = iota((4 * size, size), 0), iota((4 * size, size), 1)
    move = [ones_where((c == 2 * (r // 8) + r % 2) & ((r % 8) // 2 == q)) for q in range(4)]
    r, c = iota((4 * size, LANES), 0), iota((4 * size, LANES), 1)
    source = jnp.where(r % 8 == 6, ((r // 8) % tensor) * askers + r // capacity, -LANES)
    blocks = n_slots // size
    outs = []
    for b in range(blocks):
        if b % (blocks // 2) == 0:
            h = b // (blocks // 2)
            pltpu.make_async_copy(
                table_hbm.at[pl.ds(0, half * 2), :],
                groups.at[pl.ds(h * half * 2, half * 2), :],
                sems.at[1 + h],
            ).wait()
        pick = ones_where(offset == column[b * size : (b + 1) * size, :])
        rows = mm(pick, groups[b * 2 * size : (b + 1) * 2 * size, :]).astype(BF16)
        full = mm(move[0], rows[:, :width])
        for q in (1, 2):
            full = full + mm(move[q], rows[:, q * width : (q + 1) * width])
        tail = mm(move[3], rows[:, 3 * width : emb])
        squares = mm(ones_where(c == source + b * (size // slots)), extra)
        full = jnp.concatenate(
            [full[:, :LANES] + tail, full[:, LANES : 2 * LANES] + squares, full[:, 2 * LANES :]],
            axis=1,
        )
        span = pl.ds(b * size // 2, size // 2)
        out_ref[b * size // 2 : (b + 1) * size // 2] = full.astype(BF16).reshape(size // 2, 8, width)
        outs.append(pltpu.make_async_copy(out_ref.at[span], out_hbm.at[span], sems.at[3 + b]))
        outs[-1].start()
    for out in outs:
        out.wait()


def attention_kernel(
    lens_ref, ids_ref, x_ref, qw_hbm, kvw_hbm, key_hbm, val_hbm, ow_hbm,
    out_ref, map_ref, qw, kvw, key, val, ow, sems, *, mapping,
):
    seqs, width = x_ref.shape
    ctx_len = key_hbm.shape[1]
    heads = qw_hbm.shape[1] // HEAD_DIM
    pad = 8
    copies = [
        pltpu.make_async_copy(src, dst, sems.at[i])
        for i, (src, dst) in enumerate(
            (
                (qw_hbm, qw),
                (kvw_hbm, kvw),
                (key_hbm, key),
                (val_hbm, val),
                (ow_hbm, ow),
            )
        )
    ]
    for copy in copies:
        copy.start()
    slot_map_kernel(ids_ref, map_ref, **mapping)
    x = x_ref[...]
    copies[0].wait()
    query = mm(x, qw[...]).astype(BF16)
    src, dst = iota((HEAD_DIM, 4 * HEAD_DIM), 0), iota((HEAD_DIM, 4 * HEAD_DIM), 1)
    spread = ones_where(dst - jnp.where(dst < 2 * HEAD_DIM, 0, 2 * HEAD_DIM + 1) == 2 * src)
    blocks = width // HEAD_DIM
    stacked = jnp.concatenate(
        [x[:, g * HEAD_DIM : (g + 1) * HEAD_DIM] for g in range(blocks)], axis=0
    )
    wide = mm(stacked, spread).astype(BF16)
    even = jnp.concatenate(
        [wide[g * seqs : (g + 1) * seqs, : 2 * HEAD_DIM] for g in range(blocks)], axis=1
    )
    odd = jnp.concatenate(
        [wide[g * seqs : (g + 1) * seqs, 2 * HEAD_DIM :] for g in range(blocks)], axis=1
    )
    copies[1].wait()
    new_kv = mm(jnp.concatenate([even, odd], axis=0), kvw[...]).astype(BF16)
    rows = seqs * pad
    r, c = iota((rows, seqs), 0), iota((rows, seqs), 1)
    q_rows = jnp.zeros((rows, HEAD_DIM), F32)
    for g in range(heads):
        put = ones_where((r // pad == c) & (r % pad == g))
        q_rows = q_rows + mm(put, query[:, g * HEAD_DIM : (g + 1) * HEAD_DIM])
    rep = ones_where(r // pad == c)
    new_key = mm(rep, new_kv[:seqs, :])
    new_value = mm(rep, new_kv[seqs:, :])
    inv_scale = 1.0 / math.sqrt(HEAD_DIM)
    own = jnp.sum(q_rows * new_key, axis=1, keepdims=True) * inv_scale
    copies[2].wait()
    place = iota((pad, ctx_len), 1)
    energies = []
    for s in range(seqs):
        q_s = q_rows[s * pad : (s + 1) * pad, :].astype(BF16)
        score = mm_nt(q_s, key[s]) * inv_scale
        energies.append(jnp.where(place < lens_ref[s], score, -1e30))
    energies = jnp.concatenate(energies, axis=0)
    top = jnp.maximum(jnp.max(energies, axis=1, keepdims=True), own)
    weights = jnp.exp(energies - top)
    own_weight = jnp.exp(own - top)
    denom = jnp.sum(weights, axis=1, keepdims=True) + own_weight
    probs = weights / denom
    own_prob = (own_weight / denom).astype(BF16).astype(F32)
    copies[3].wait()
    context = []
    for s in range(seqs):
        context.append(mm(probs[s * pad : (s + 1) * pad, :].astype(BF16), val[s]))
    context = (jnp.concatenate(context, axis=0) + own_prob * new_value).astype(BF16)
    r, c = iota((seqs, rows), 0), iota((seqs, rows), 1)
    flat = []
    for g in range(heads):
        take = ones_where((c // pad == r) & (c % pad == g))
        flat.append(mm(take, context).astype(BF16))
    copies[4].wait()
    out_ref[...] = mm(jnp.concatenate(flat, axis=1), ow[...]).astype(BF16)


def mix_kernel(got_ref, map_ref, u_ref, more_u_ref, attn_ref, out_ref, *, width):
    total, columns = map_ref.shape
    seqs, emb = u_ref.shape
    part = got_ref.shape[2]
    rows = got_ref[...].reshape(total, part)
    of_seq = map_ref[...].astype(F32)
    u = u_ref[...].astype(F32) + more_u_ref[...].astype(F32)
    parts = columns // seqs
    u = jnp.concatenate([u, jnp.zeros((seqs, parts * part - emb), F32)], axis=1)
    u = jnp.concatenate([u[:, q * part : (q + 1) * part] for q in range(parts)], axis=0)
    u_high, u_low = two_parts(u)
    cross_all = (mm_nt(rows, u_high) + mm_nt(rows, u_low)) * of_seq
    r, c = iota((LANES, LANES), 0), iota((LANES, LANES), 1)
    same = ones_where((r // 8 == c // 8) & (r % 2 == c % 2))
    sums = []
    for b in range(0, total, LANES):
        high, mid, low = three_parts(cross_all[b : b + LANES, :])
        sums.append(mm(same, high) + (mm(same, mid) + mm(same, low)))
    cross = jnp.sum(jnp.concatenate(sums, axis=0), axis=1, keepdims=True)
    owners = total // 32
    row = iota((total, LANES), 0)
    extra = jnp.where(row % 8 == 6, rows[:, LANES : 2 * LANES].astype(F32), 0.0)
    extra = jnp.sum(extra.reshape(owners, 32, LANES), axis=1)
    square = extra + (pltpu.roll(extra, LANES - 8, 1) + pltpu.roll(extra, LANES - 16, 1))
    spread = jnp.broadcast_to(square[:, None, :], (owners, 32, LANES)).reshape(total, LANES)
    place = row % 32
    keep = iota((total, LANES), 1) == (place // 8) * 2 + place % 2
    square = jnp.sum(jnp.where(keep, spread, 0.0), axis=1, keepdims=True)
    gate = jax.nn.sigmoid(cross * lax.rsqrt(square / width + EPS) / math.sqrt(width))
    g_high, g_low = two_parts(of_seq * gate)
    mixed = mm_tn(g_high, rows) + mm_tn(g_low, rows)
    mixed = jnp.concatenate([mixed[q * seqs : (q + 1) * seqs, :] for q in range(parts)], axis=1)
    mixed = mixed[:, :emb].astype(BF16)
    peers = out_ref.shape[0]
    own = width // peers
    for p in range(peers):
        out_ref[p, :, :own] = attn_ref[:, p * own : (p + 1) * own]
        out_ref[p, :, own:] = mixed


def fetch_kernel(value_hbm, hidden_hbm, order_ref, value_ref, hidden_ref, sems):
    del order_ref
    copies = [
        pltpu.make_async_copy(value_hbm, value_ref, sems.at[0]),
        pltpu.make_async_copy(hidden_hbm, hidden_ref, sems.at[1]),
    ]
    for copy in copies:
        copy.start()
    for copy in copies:
        copy.wait()


def final_kernel(got_ref, value_ref, hidden_ref, out_ref):
    part = out_ref.shape[1]
    first = pl.multiple_of(lax.axis_index("tensor") * part, LANES)
    total = got_ref[0].astype(F32)
    for p in range(1, got_ref.shape[0]):
        total = total + got_ref[p].astype(F32)
    high, low = two_parts(total[:, part:])
    memory = mm(high, value_ref[...]) + mm(low, value_ref[...])
    out_ref[...] = (hidden_ref[:, pl.ds(first, part)].astype(F32) + total[:, :part] + memory).astype(BF16)


def body(
    hidden,
    attn_gain,
    q_weight,
    kv_weight,
    out_weight,
    key_cache,
    value_cache,
    cache_lengths,
    table,
    key_proj,
    value_proj,
    lookup_ids,
):
    seqs, width = hidden.shape
    lookups = lookup_ids.shape[1]
    requests = seqs * lookups
    rows_dev, emb = table.shape
    owners = lax.axis_size("table")
    tensor = lax.axis_size("tensor")
    part = width // tensor
    capacity = 2 * requests // owners
    slots = capacity // tensor
    n_slots = owners * slots
    per = requests // LANES

    vmem = pl.BlockSpec(memory_space=pltpu.VMEM)
    smem = pl.BlockSpec(memory_space=pltpu.SMEM)
    hbm = pl.BlockSpec(memory_space=pl.ANY)
    ids_t = lookup_ids.T

    def near(x):
        return pltpu.with_memory_space_constraint(x, pltpu.VMEM)

    def other(x, step):
        return lax.ppermute(x, "tensor", [(i, i ^ step) for i in range(tensor)])

    send, u, attn_in, key_t = pl.pallas_call(
        start_kernel,
        in_specs=[hbm] * 4,
        out_specs=[hbm] + [vmem] * 3,
        out_shape=[
            jax.ShapeDtypeStruct((owners, per, LANES), I32),
            pltpu.VMEM((seqs, emb), BF16),
            pltpu.VMEM(hidden.shape, BF16),
            pltpu.VMEM((part, emb), BF16),
        ],
        scratch_shapes=[
            pltpu.VMEM(ids_t.shape, I32),
            pltpu.VMEM(attn_gain.shape, F32),
            pltpu.VMEM(hidden.shape, BF16),
            pltpu.VMEM(key_proj.shape, BF16),
            pltpu.VMEM((owners, per, LANES), I32),
            pltpu.SemaphoreType.DMA((5,)),
        ],
        name="start",
    )(ids_t, attn_gain, hidden, key_proj)
    more_u = other(u, 1)
    got_ids = lax.all_to_all(send, "table", 0, 0, tiled=True)

    u = (u.astype(F32) + more_u.astype(F32)).astype(BF16)
    more_u = other(u, 2)

    chunks = (256, 256, 512, 1024)
    more_chunks = (1024, 1024)
    early_rows = sum(chunks)
    squares = pl.pallas_call(
        lambda *refs: squares_kernel(*refs, chunks=chunks),
        in_specs=[vmem, hbm],
        out_specs=vmem,
        out_shape=pltpu.VMEM((early_rows // LANES, LANES), F32),
        scratch_shapes=[
            pltpu.VMEM((early_rows, emb), BF16),
            pltpu.SemaphoreType.DMA((len(chunks),)),
        ],
        name="squares",
    )(near(key_t), table)

    packed = pl.pallas_call(
        lambda *refs: gather_kernel(
            *refs, rows_dev=rows_dev, per=per, capacity=capacity, tensor=tensor, chunks=more_chunks
        ),
        in_specs=[vmem, vmem, vmem, hbm],
        out_specs=hbm,
        out_shape=jax.ShapeDtypeStruct((owners * tensor, 8, 3 * LANES), BF16),
        scratch_shapes=[
            pltpu.VMEM((n_slots // LANES, LANES), I32),
            pltpu.SMEM((n_slots // LANES, LANES), I32),
            pltpu.VMEM((n_slots * 2, emb), BF16),
            pltpu.VMEM((owners * tensor, 8, 3 * LANES), BF16),
            pltpu.VMEM((rows_dev - early_rows, emb), BF16),
            pltpu.VMEM((rows_dev // LANES, LANES), F32),
            pltpu.SemaphoreType.DMA((11,)),
            pltpu.SemaphoreType.DMA((len(more_chunks),)),
        ],
        name="gather",
    )(near(got_ids.reshape(owners * per, LANES)), near(squares), near(key_t), table)
    got_rows = lax.all_to_all(packed, ("table", "tensor"), 0, 0, tiled=True)
    _, kv_width = key_cache.shape[1:]
    mapping = dict(rows_dev=rows_dev, owners=owners, seqs=seqs, lookups=lookups, capacity=capacity, tensor=tensor)
    attention, slot_map = pl.pallas_call(
        lambda *refs: attention_kernel(*refs, mapping=mapping),
        in_specs=[smem, vmem, vmem, hbm, hbm, hbm, hbm, hbm],
        out_specs=[vmem, vmem],
        out_shape=[
            pltpu.VMEM((seqs, width), BF16),
            pltpu.VMEM((4 * n_slots, 4 * seqs), BF16),
        ],
        scratch_shapes=[
            pltpu.VMEM(q_weight.shape, BF16),
            pltpu.VMEM((2 * width, kv_width), BF16),
            pltpu.VMEM(key_cache.shape, BF16),
            pltpu.VMEM(value_cache.shape, BF16),
            pltpu.VMEM(out_weight.shape, BF16),
            pltpu.SemaphoreType.DMA((5,)),
        ],
        name="attention",
    )(
        cache_lengths, ids_t, near(attn_in), q_weight,
        kv_weight.reshape(2 * width, kv_width), key_cache, value_cache, out_weight,
    )

    mixes = pl.pallas_call(
        lambda *refs: mix_kernel(*refs, width=width),
        in_specs=[vmem] * 5,
        out_specs=vmem,
        out_shape=jax.ShapeDtypeStruct((tensor, seqs, part + emb), BF16),
        name="mix",
    )(near(got_rows), near(slot_map), near(u), near(more_u), near(attention))
    got_mixes = lax.all_to_all(mixes, "tensor", 0, 0, tiled=True)

    value_near, hidden_near = pl.pallas_call(
        fetch_kernel,
        in_specs=[hbm] * 3,
        out_specs=[vmem] * 2,
        out_shape=[pltpu.VMEM(value_proj.shape, BF16), pltpu.VMEM(hidden.shape, BF16)],
        scratch_shapes=[pltpu.SemaphoreType.DMA((2,))],
        name="fetch_value",
    )(value_proj, hidden, mixes)

    return pl.pallas_call(
        final_kernel,
        in_specs=[vmem] * 3,
        out_specs=vmem,
        out_shape=jax.ShapeDtypeStruct((seqs, part), BF16),
        name="final",
    )(near(got_mixes), near(value_near), near(hidden_near))


def solution(mesh):
    return jax.shard_map(
        body,
        mesh=mesh,
        in_specs=(
            P("table", None),
            P(),
            P(None, "tensor"),
            P(None, None, "tensor"),
            P("tensor", None),
            P("table", None, "tensor"),
            P("table", None, "tensor"),
            P("table"),
            P("table", None),
            P(None, "tensor"),
            P(None, "tensor"),
            P("table", None),
        ),
        out_specs=P("table", "tensor"),
        check_vma=False,
    )
```

```python
import math

import jax
import jax.numpy as jnp
from jax import lax
from jax.experimental import pallas as pl
from jax.experimental.pallas import tpu as pltpu
from jax.sharding import PartitionSpec as P


HEAD_DIM = 128
EPS = 1e-06
LANES = 128
F32 = jnp.float32
BF16 = jnp.bfloat16
I32 = jnp.int32


def iota(shape, dim):
    return lax.broadcasted_iota(I32, shape, dim)


def ones_where(mask):
    return jnp.where(mask, 1.0, 0.0).astype(BF16)


def mm(a, b):
    return lax.dot_general(a, b, (((1,), (0,)), ((), ())), preferred_element_type=F32)


def mm_nt(a, b):
    return lax.dot_general(a, b, (((1,), (1,)), ((), ())), preferred_element_type=F32)


def mm_tn(a, b):
    return lax.dot_general(a, b, (((0,), (0,)), ((), ())), preferred_element_type=F32)


def two_parts(x):
    high = x.astype(BF16)
    return high, (x - high.astype(F32)).astype(BF16)


def three_parts(x):
    high = x.astype(BF16)
    rest = x - high.astype(F32)
    mid = rest.astype(BF16)
    return high, mid, (rest - mid.astype(F32)).astype(BF16)


def start_kernel(
    ids_hbm, gain_hbm, hidden_hbm, key_hbm, send_hbm, u_ref, attn_in_ref, key_t,
    ids_ref, gain_ref, hidden_ref, key_ref, send_ref, sems,
):
    copies = [
        pltpu.make_async_copy(src, dst, sems.at[i])
        for i, (src, dst) in enumerate(
            ((ids_hbm, ids_ref), (hidden_hbm, hidden_ref), (gain_hbm, gain_ref), (key_hbm, key_ref))
        )
    ]
    for copy in copies:
        copy.start()
    _, per, _ = send_ref.shape
    _, seqs = ids_ref.shape
    fit = LANES // seqs
    copies[0].wait()
    flat = [
        jnp.concatenate([ids_ref[j * fit + q : j * fit + q + 1, :] for q in range(fit)], axis=1)
        for j in range(per)
    ]
    send_ref[...] = jnp.broadcast_to(jnp.concatenate(flat, axis=0)[None], send_ref.shape)
    out = pltpu.make_async_copy(send_ref, send_hbm, sems.at[4])
    out.start()
    copies[1].wait()
    part = key_ref.shape[1]
    hidden = hidden_ref[...].astype(F32)
    inv = lax.rsqrt(jnp.mean(hidden * hidden, axis=1, keepdims=True) + EPS)
    copies[2].wait()
    attn_in_ref[...] = (hidden * inv * gain_ref[...].reshape(1, hidden.shape[1])).astype(BF16)
    first = pl.multiple_of(lax.axis_index("tensor") * part, LANES)
    high, low = two_parts(hidden_ref[:, pl.ds(first, part)].astype(F32) * inv)
    copies[3].wait()
    key_t[...] = key_ref[...].T
    u = mm(jnp.concatenate([high, low], axis=0), key_t[...])
    u_ref[...] = (u[:seqs] + u[seqs:]).astype(BF16)
    out.wait()


def slot_map_kernel(ids_ref, map_ref, *, rows_dev, owners, seqs, lookups, capacity, tensor):
    requests = seqs * lookups
    total, width = map_ref.shape
    ids = jnp.concatenate([ids_ref[j : j + 1, :] for j in range(lookups)], axis=1)
    owner = ids // rows_dev
    hit = ones_where(iota((owners, requests), 0) == owner)
    before = ones_where(iota((requests, requests), 0) < iota((requests, requests), 1))
    rank = jnp.sum(mm(hit, before) * hit.astype(F32), axis=0, keepdims=True).astype(I32)
    key = owner * capacity + rank - lax.axis_index("tensor") * (capacity // tensor)
    row = iota((total, requests), 0)
    place = row % capacity
    placed = ones_where(row - place + (place // 8) * 2 + place % 2 == key)
    of_seq = ones_where(iota((width, requests), 1) % seqs == iota((width, requests), 0) % seqs)
    part = (iota((total, width), 0) % 8) // 2
    known = mm_nt(placed, of_seq)
    map_ref[...] = jnp.where(part == iota((total, width), 1) // seqs, known, 0.0).astype(BF16)


def fetch_rows(table_hbm, table, sems, first, chunks):
    copies, start = [], 0
    for i, size in enumerate(chunks):
        copies.append(
            pltpu.make_async_copy(
                table_hbm.at[pl.ds(first + start, size), :],
                table.at[pl.ds(start, size), :],
                sems.at[i],
            )
        )
        copies[-1].start()
        start += size
    return copies


def row_squares(key_t, table, squares, copies, first, chunks, between=None):
    sub, start = 256, 0
    for copy, size in zip(copies, chunks):
        copy.wait()
        for t in range(start, start + size, sub):
            if between is not None and t == 0:
                for i in range(4):
                    between(i)
            keys = mm_nt(key_t[...], table[t : t + sub, :])
            line = jnp.sum(keys * keys, axis=0, keepdims=True)
            for g in range(sub // LANES):
                group = (first + t) // LANES + g
                squares[group : group + 1, :] = line[:, g * LANES : (g + 1) * LANES]
        start += size


def squares_kernel(key_t, table_hbm, squares, table, sems, *, chunks):
    row_squares(key_t, table, squares, fetch_rows(table_hbm, table, sems, 0, chunks), 0, chunks)


def slot_lanes(row, z, slots):
    askers = row.shape[0]
    lane = iota((askers, LANES), 1)
    own = row if z == 0 else pltpu.roll(row, LANES - z * slots, 1)
    own = jnp.where(lane < slots, own, 0.0)
    step = slots
    while step < LANES:
        own = own + pltpu.roll(own, step, 1)
        step *= 2
    fit = LANES // slots
    own = jnp.where(lane // slots == iota((askers, LANES), 0) % fit, own, 0.0)
    return jnp.sum(own.reshape(askers // fit, fit, LANES), axis=1)


def gather_kernel(
    got_ref, some_ref, key_t, table_hbm, out_hbm,
    idx_vmem, idx_smem, groups, out_ref, table, sq_ref, sems, table_sems,
    *, rows_dev, per, capacity, tensor, chunks,
):
    askers = got_ref.shape[0] // per
    slots = capacity // tensor
    n_slots = askers * slots
    me, mine_z = lax.axis_index("table"), lax.axis_index("tensor")
    done = some_ref.shape[0]
    copies = fetch_rows(table_hbm, table, table_sems, done * LANES, chunks)
    sq_ref[:done, :] = some_ref[...]
    before = ones_where(iota((LANES, LANES), 0) < iota((LANES, LANES), 1))
    lane = iota((askers, LANES), 1)
    seen = jnp.zeros((askers, 1), F32)
    ranks, locals_ = [], []
    for j in range(per):
        local = got_ref[pl.ds(j, askers, stride=per), :] - me * rows_dev
        mine = (local >= 0) & (local < rows_dev)
        rank = mm(ones_where(mine), before) + seen
        seen = seen + jnp.sum(jnp.where(mine, 1.0, 0.0), axis=1, keepdims=True)
        ranks.append(jnp.where(mine, rank, -1.0).astype(I32))
        locals_.append(local.astype(F32))

    def ranked(target):
        one = jnp.where(ranks[0] == target, locals_[0], 0.0)
        for j in range(1, per):
            one = one + jnp.where(ranks[j] == target, locals_[j], 0.0)
        return jnp.sum(one, axis=1, keepdims=True)

    own = jnp.zeros((askers, LANES), F32)
    for k in range(slots):
        own = jnp.where(lane == k, ranked((k // 2) * slots + k % 2 + 2 * mine_z), own)
    idx_vmem[...] = slot_lanes(own, 0, slots).astype(I32)
    to_smem = pltpu.make_async_copy(idx_vmem, idx_smem, sems.at[0])
    to_smem.start()
    row = jnp.zeros((askers, LANES), F32)
    for k in range(capacity):
        row = jnp.where(lane == k, ranked(k), row)
    to_smem.wait()
    half = n_slots // 2
    steps = 4
    each = n_slots // steps

    def issue(step):
        for s in range(step * each, (step + 1) * each):
            base = pl.multiple_of((idx_smem[s // LANES, s % LANES] // 2) * 2, 2)
            pltpu.make_async_copy(
                table_hbm.at[pl.ds(base, 2), :],
                groups.at[pl.ds(s * 2, 2), :],
                sems.at[1 + s // half],
            ).start()

    row_squares(key_t, table, sq_ref, copies, done * LANES, chunks, issue)
    ids = row.astype(I32)
    high, low = ids // LANES, ids % LANES
    value = jnp.zeros((askers, LANES), F32)
    for g in range(sq_ref.shape[0]):
        line = jnp.broadcast_to(sq_ref[g : g + 1, :], (askers, LANES))
        found = jnp.take_along_axis(line, low, axis=1, mode="promise_in_bounds")
        value = jnp.where(high == g, found, value)
    extra = []
    for z in range(tensor):
        piece = value if z == 0 else pltpu.roll(value, LANES - slots * z, 1)
        line = jnp.zeros((askers, LANES), F32)
        for p, part in enumerate(three_parts(jnp.where(lane < slots, piece, 0.0))):
            part = part.astype(F32)
            line = line + (part if p == 0 else pltpu.roll(part, slots * p, 1))
        extra.append(line.astype(BF16))
    extra = jnp.concatenate(extra, axis=0)
    spread = jnp.broadcast_to((own.astype(I32) % 2)[:, None, :], (askers, slots, LANES))
    spread = spread.reshape(n_slots, LANES).astype(F32)
    keep = iota((n_slots, LANES), 1) == iota((n_slots, LANES), 0) % slots
    column = jnp.sum(jnp.where(keep, spread, 0.0), axis=1, keepdims=True)
    size = 64
    width = out_ref.shape[2]
    emb = groups.shape[1]
    offset = (iota((size, 2 * size), 1) - 2 * iota((size, 2 * size), 0)).astype(F32)
    r, c = iota((4 * size, size), 0), iota((4 * size, size), 1)
    move = [ones_where((c == 2 * (r // 8) + r % 2) & ((r % 8) // 2 == q)) for q in range(4)]
    r, c = iota((4 * size, LANES), 0), iota((4 * size, LANES), 1)
    source = jnp.where(r % 8 == 6, ((r // 8) % tensor) * askers + r // capacity, -LANES)
    blocks = n_slots // size
    outs = []
    for b in range(blocks):
        if b % (blocks // 2) == 0:
            h = b // (blocks // 2)
            pltpu.make_async_copy(
                table_hbm.at[pl.ds(0, half * 2), :],
                groups.at[pl.ds(h * half * 2, half * 2), :],
                sems.at[1 + h],
            ).wait()
        pick = ones_where(offset == column[b * size : (b + 1) * size, :])
        rows = mm(pick, groups[b * 2 * size : (b + 1) * 2 * size, :]).astype(BF16)
        full = mm(move[0], rows[:, :width])
        for q in (1, 2):
            full = full + mm(move[q], rows[:, q * width : (q + 1) * width])
        tail = mm(move[3], rows[:, 3 * width : emb])
        squares = mm(ones_where(c == source + b * (size // slots)), extra)
        full = jnp.concatenate(
            [full[:, :LANES] + tail, full[:, LANES : 2 * LANES] + squares, full[:, 2 * LANES :]],
            axis=1,
        )
        span = pl.ds(b * size // 2, size // 2)
        out_ref[b * size // 2 : (b + 1) * size // 2] = full.astype(BF16).reshape(size // 2, 8, width)
        outs.append(pltpu.make_async_copy(out_ref.at[span], out_hbm.at[span], sems.at[3 + b]))
        outs[-1].start()
    for out in outs:
        out.wait()


def attention_kernel(
    lens_ref, ids_ref, x_ref, qw_hbm, kvw_hbm, key_hbm, val_hbm, ow_hbm,
    out_ref, map_ref, qw, kvw, key, val, ow, sems, *, mapping,
):
    seqs, width = x_ref.shape
    ctx_len = key_hbm.shape[1]
    heads = qw_hbm.shape[1] // HEAD_DIM
    pad = 8
    copies = [
        pltpu.make_async_copy(src, dst, sems.at[i])
        for i, (src, dst) in enumerate(
            (
                (qw_hbm, qw),
                (kvw_hbm, kvw),
                (key_hbm, key),
                (val_hbm, val),
                (ow_hbm, ow),
            )
        )
    ]
    for copy in copies:
        copy.start()
    slot_map_kernel(ids_ref, map_ref, **mapping)
    x = x_ref[...]
    copies[0].wait()
    query = mm(x, qw[...]).astype(BF16)
    src, dst = iota((HEAD_DIM, 4 * HEAD_DIM), 0), iota((HEAD_DIM, 4 * HEAD_DIM), 1)
    spread = ones_where(dst - jnp.where(dst < 2 * HEAD_DIM, 0, 2 * HEAD_DIM + 1) == 2 * src)
    blocks = width // HEAD_DIM
    stacked = jnp.concatenate(
        [x[:, g * HEAD_DIM : (g + 1) * HEAD_DIM] for g in range(blocks)], axis=0
    )
    wide = mm(stacked, spread).astype(BF16)
    even = jnp.concatenate(
        [wide[g * seqs : (g + 1) * seqs, : 2 * HEAD_DIM] for g in range(blocks)], axis=1
    )
    odd = jnp.concatenate(
        [wide[g * seqs : (g + 1) * seqs, 2 * HEAD_DIM :] for g in range(blocks)], axis=1
    )
    copies[1].wait()
    new_kv = mm(jnp.concatenate([even, odd], axis=0), kvw[...]).astype(BF16)
    rows = seqs * pad
    r, c = iota((rows, seqs), 0), iota((rows, seqs), 1)
    q_rows = jnp.zeros((rows, HEAD_DIM), F32)
    for g in range(heads):
        put = ones_where((r // pad == c) & (r % pad == g))
        q_rows = q_rows + mm(put, query[:, g * HEAD_DIM : (g + 1) * HEAD_DIM])
    rep = ones_where(r // pad == c)
    new_key = mm(rep, new_kv[:seqs, :])
    new_value = mm(rep, new_kv[seqs:, :])
    inv_scale = 1.0 / math.sqrt(HEAD_DIM)
    own = jnp.sum(q_rows * new_key, axis=1, keepdims=True) * inv_scale
    copies[2].wait()
    place = iota((pad, ctx_len), 1)
    energies = []
    for s in range(seqs):
        q_s = q_rows[s * pad : (s + 1) * pad, :].astype(BF16)
        score = mm_nt(q_s, key[s]) * inv_scale
        energies.append(jnp.where(place < lens_ref[s], score, -1e30))
    energies = jnp.concatenate(energies, axis=0)
    top = jnp.maximum(jnp.max(energies, axis=1, keepdims=True), own)
    weights = jnp.exp(energies - top)
    own_weight = jnp.exp(own - top)
    denom = jnp.sum(weights, axis=1, keepdims=True) + own_weight
    probs = weights / denom
    own_prob = (own_weight / denom).astype(BF16).astype(F32)
    copies[3].wait()
    context = []
    for s in range(seqs):
        context.append(mm(probs[s * pad : (s + 1) * pad, :].astype(BF16), val[s]))
    context = (jnp.concatenate(context, axis=0) + own_prob * new_value).astype(BF16)
    r, c = iota((seqs, rows), 0), iota((seqs, rows), 1)
    flat = []
    for g in range(heads):
        take = ones_where((c // pad == r) & (c % pad == g))
        flat.append(mm(take, context).astype(BF16))
    copies[4].wait()
    out_ref[...] = mm(jnp.concatenate(flat, axis=1), ow[...]).astype(BF16)


def mix_kernel(got_ref, map_ref, u_ref, more_u_ref, attn_ref, out_ref, *, width):
    total, columns = map_ref.shape
    seqs, emb = u_ref.shape
    part = got_ref.shape[2]
    rows = got_ref[...].reshape(total, part)
    of_seq = map_ref[...].astype(F32)
    u = u_ref[...].astype(F32) + more_u_ref[...].astype(F32)
    parts = columns // seqs
    u = jnp.concatenate([u, jnp.zeros((seqs, parts * part - emb), F32)], axis=1)
    u = jnp.concatenate([u[:, q * part : (q + 1) * part] for q in range(parts)], axis=0)
    u_high, u_low = two_parts(u)
    cross_all = (mm_nt(rows, u_high) + mm_nt(rows, u_low)) * of_seq
    r, c = iota((LANES, LANES), 0), iota((LANES, LANES), 1)
    same = ones_where((r // 8 == c // 8) & (r % 2 == c % 2))
    sums = []
    for b in range(0, total, LANES):
        high, low = two_parts(cross_all[b : b + LANES, :])
        sums.append(mm(same, high) + mm(same, low))
    cross = jnp.sum(jnp.concatenate(sums, axis=0), axis=1, keepdims=True)
    owners = total // 32
    row = iota((total, LANES), 0)
    extra = jnp.where(row % 8 == 6, rows[:, LANES : 2 * LANES].astype(F32), 0.0)
    extra = jnp.sum(extra.reshape(owners, 32, LANES), axis=1)
    square = extra + (pltpu.roll(extra, LANES - 8, 1) + pltpu.roll(extra, LANES - 16, 1))
    spread = jnp.broadcast_to(square[:, None, :], (owners, 32, LANES)).reshape(total, LANES)
    place = row % 32
    keep = iota((total, LANES), 1) == (place // 8) * 2 + place % 2
    square = jnp.sum(jnp.where(keep, spread, 0.0), axis=1, keepdims=True)
    gate = jax.nn.sigmoid(cross * lax.rsqrt(square / width + EPS) / math.sqrt(width))
    g_high, g_low = two_parts(of_seq * gate)
    mixed = mm_tn(g_high, rows) + mm_tn(g_low, rows)
    mixed = jnp.concatenate([mixed[q * seqs : (q + 1) * seqs, :] for q in range(parts)], axis=1)
    mixed = mixed[:, :emb].astype(BF16)
    peers = out_ref.shape[0]
    own = width // peers
    for p in range(peers):
        out_ref[p, :, :own] = attn_ref[:, p * own : (p + 1) * own]
        out_ref[p, :, own:] = mixed


def fetch_kernel(value_hbm, hidden_hbm, order_ref, value_ref, hidden_ref, sems):
    del order_ref
    copies = [
        pltpu.make_async_copy(value_hbm, value_ref, sems.at[0]),
        pltpu.make_async_copy(hidden_hbm, hidden_ref, sems.at[1]),
    ]
    for copy in copies:
        copy.start()
    for copy in copies:
        copy.wait()


def final_kernel(got_ref, value_ref, hidden_ref, out_ref):
    part = out_ref.shape[1]
    first = pl.multiple_of(lax.axis_index("tensor") * part, LANES)
    total = got_ref[0].astype(F32)
    for p in range(1, got_ref.shape[0]):
        total = total + got_ref[p].astype(F32)
    high, low = two_parts(total[:, part:])
    memory = mm(high, value_ref[...]) + mm(low, value_ref[...])
    out_ref[...] = (hidden_ref[:, pl.ds(first, part)].astype(F32) + total[:, :part] + memory).astype(BF16)


def body(
    hidden,
    attn_gain,
    q_weight,
    kv_weight,
    out_weight,
    key_cache,
    value_cache,
    cache_lengths,
    table,
    key_proj,
    value_proj,
    lookup_ids,
):
    seqs, width = hidden.shape
    lookups = lookup_ids.shape[1]
    requests = seqs * lookups
    rows_dev, emb = table.shape
    owners = lax.axis_size("table")
    tensor = lax.axis_size("tensor")
    part = width // tensor
    capacity = 2 * requests // owners
    slots = capacity // tensor
    n_slots = owners * slots
    per = requests // LANES

    vmem = pl.BlockSpec(memory_space=pltpu.VMEM)
    smem = pl.BlockSpec(memory_space=pltpu.SMEM)
    hbm = pl.BlockSpec(memory_space=pl.ANY)
    ids_t = lookup_ids.T

    def near(x):
        return pltpu.with_memory_space_constraint(x, pltpu.VMEM)

    def other(x, step):
        return lax.ppermute(x, "tensor", [(i, i ^ step) for i in range(tensor)])

    send, u, attn_in, key_t = pl.pallas_call(
        start_kernel,
        in_specs=[hbm] * 4,
        out_specs=[hbm] + [vmem] * 3,
        out_shape=[
            jax.ShapeDtypeStruct((owners, per, LANES), I32),
            pltpu.VMEM((seqs, emb), BF16),
            pltpu.VMEM(hidden.shape, BF16),
            pltpu.VMEM((part, emb), BF16),
        ],
        scratch_shapes=[
            pltpu.VMEM(ids_t.shape, I32),
            pltpu.VMEM(attn_gain.shape, F32),
            pltpu.VMEM(hidden.shape, BF16),
            pltpu.VMEM(key_proj.shape, BF16),
            pltpu.VMEM((owners, per, LANES), I32),
            pltpu.SemaphoreType.DMA((5,)),
        ],
        name="start",
    )(ids_t, attn_gain, hidden, key_proj)
    more_u = other(u, 1)
    got_ids = lax.all_to_all(send, "table", 0, 0, tiled=True)

    u = (u.astype(F32) + more_u.astype(F32)).astype(BF16)
    more_u = other(u, 2)

    chunks = (256, 512, 768)
    more_chunks = (1024, 1536)
    early_rows = sum(chunks)
    squares = pl.pallas_call(
        lambda *refs: squares_kernel(*refs, chunks=chunks),
        in_specs=[vmem, hbm],
        out_specs=vmem,
        out_shape=pltpu.VMEM((early_rows // LANES, LANES), F32),
        scratch_shapes=[
            pltpu.VMEM((early_rows, emb), BF16),
            pltpu.SemaphoreType.DMA((len(chunks),)),
        ],
        name="squares",
    )(near(key_t), table)

    packed = pl.pallas_call(
        lambda *refs: gather_kernel(
            *refs, rows_dev=rows_dev, per=per, capacity=capacity, tensor=tensor, chunks=more_chunks
        ),
        in_specs=[vmem, vmem, vmem, hbm],
        out_specs=hbm,
        out_shape=jax.ShapeDtypeStruct((owners * tensor, 8, 3 * LANES), BF16),
        scratch_shapes=[
            pltpu.VMEM((n_slots // LANES, LANES), I32),
            pltpu.SMEM((n_slots // LANES, LANES), I32),
            pltpu.VMEM((n_slots * 2, emb), BF16),
            pltpu.VMEM((owners * tensor, 8, 3 * LANES), BF16),
            pltpu.VMEM((rows_dev - early_rows, emb), BF16),
            pltpu.VMEM((rows_dev // LANES, LANES), F32),
            pltpu.SemaphoreType.DMA((11,)),
            pltpu.SemaphoreType.DMA((len(more_chunks),)),
        ],
        name="gather",
    )(near(got_ids.reshape(owners * per, LANES)), near(squares), near(key_t), table)
    got_rows = lax.all_to_all(packed, ("table", "tensor"), 0, 0, tiled=True)
    _, kv_width = key_cache.shape[1:]
    mapping = dict(rows_dev=rows_dev, owners=owners, seqs=seqs, lookups=lookups, capacity=capacity, tensor=tensor)
    attention, slot_map = pl.pallas_call(
        lambda *refs: attention_kernel(*refs, mapping=mapping),
        in_specs=[smem, vmem, vmem, hbm, hbm, hbm, hbm, hbm],
        out_specs=[vmem, vmem],
        out_shape=[
            pltpu.VMEM((seqs, width), BF16),
            pltpu.VMEM((4 * n_slots, 4 * seqs), BF16),
        ],
        scratch_shapes=[
            pltpu.VMEM(q_weight.shape, BF16),
            pltpu.VMEM((2 * width, kv_width), BF16),
            pltpu.VMEM(key_cache.shape, BF16),
            pltpu.VMEM(value_cache.shape, BF16),
            pltpu.VMEM(out_weight.shape, BF16),
            pltpu.SemaphoreType.DMA((5,)),
        ],
        name="attention",
    )(
        cache_lengths, ids_t, near(attn_in), q_weight,
        kv_weight.reshape(2 * width, kv_width), key_cache, value_cache, out_weight,
    )

    mixes = pl.pallas_call(
        lambda *refs: mix_kernel(*refs, width=width),
        in_specs=[vmem] * 5,
        out_specs=vmem,
        out_shape=jax.ShapeDtypeStruct((tensor, seqs, part + emb), BF16),
        name="mix",
    )(near(got_rows), near(slot_map), near(u), near(more_u), near(attention))
    got_mixes = lax.all_to_all(mixes, "tensor", 0, 0, tiled=True)

    value_near, hidden_near = pl.pallas_call(
        fetch_kernel,
        in_specs=[hbm] * 3,
        out_specs=[vmem] * 2,
        out_shape=[pltpu.VMEM(value_proj.shape, BF16), pltpu.VMEM(hidden.shape, BF16)],
        scratch_shapes=[pltpu.SemaphoreType.DMA((2,))],
        name="fetch_value",
    )(value_proj, hidden, mixes)

    return pl.pallas_call(
        final_kernel,
        in_specs=[vmem] * 3,
        out_specs=vmem,
        out_shape=jax.ShapeDtypeStruct((seqs, part), BF16),
        name="final",
    )(near(got_mixes), near(value_near), near(hidden_near))


def solution(mesh):
    return jax.shard_map(
        body,
        mesh=mesh,
        in_specs=(
            P("table", None),
            P(),
            P(None, "tensor"),
            P(None, None, "tensor"),
            P("tensor", None),
            P("table", None, "tensor"),
            P("table", None, "tensor"),
            P("table"),
            P("table", None),
            P(None, "tensor"),
            P(None, "tensor"),
            P("table", None),
        ),
        out_specs=P("table", "tensor"),
        check_vma=False,
    )
```
